32 devices in a mesh: row: 8 (over z, x), col: 4 (over y, core).
Axes of the slice: x: 2, y: 2, z: 4, core: 2. Of those that a mesh axis runs over, the one named last changes fastest.
Arguments:
- queries: bfloat16 [8192, 2048], P(('row', 'col')), may hold values from -200 to 200
- keys: bfloat16 [8192, 512], P(('row', 'col')), may hold values from -6 to 6
- values: bfloat16 [8192, 512], P(('row', 'col')), may hold values from -6 to 6
- mid_key_weight: bfloat16 [1024, 128], replicated, may hold values from -0.1875 to 0.1875
- mid_value_weight: bfloat16 [1024, 128], replicated, may hold values from -0.1875 to 0.1875
- far_key_weight: bfloat16 [2048, 128], replicated, may hold values from -0.125 to 0.125
- far_value_weight: bfloat16 [2048, 128], replicated, may hold values from -0.125 to 0.125
Outputs:
- attended: bfloat16 [8192, 2048], P(('row', 'col'))
The draws below stay inside these ranges and needn't reach their ends.
All inputs are finite; a program needn't handle non-finite values.
Results may differ from the reference program's by a relative error of at most 0.012.
Values may be sent and summed in bfloat16 or wider, within the bound.
A program may use at most 128 MiB of HBM per device.

```python
import jax
import jax.numpy as jnp
from jax import lax

HQ = 16
HK = 4
DH = 128
BLOCK = 512
MID = 8
FAR = 16
TOK_DEV = 256
TOKENS = 8192
N_ROW = 8
N_COL = 4
DEVICES = 32


def draw_queries(key, part):
    key_one = jax.random.fold_in(key, 0)
    normal_part = jnp.clip(jax.random.normal(key_one, (TOKENS, HQ * DH), jnp.float32), -6.0, 6.0)
    return (1.5 * normal_part).astype(jnp.bfloat16)


def block_levels(own_key, extent, cuts, low, largest):
    factor_of, own = 1.0, jax.random.fold_in(own_key, 6)
    for axis_at, shards_of in cuts:
        heights = jnp.exp(jax.random.uniform(jax.random.fold_in(own, axis_at), (shards_of,), jnp.float32, low / len(cuts), largest / len(cuts)))
        factor_of = factor_of * jnp.repeat(heights, extent[axis_at] // shards_of).reshape([-1 if axis == axis_at else 1 for axis in range(len(extent))])
    return factor_of


def centred(own_key, shape, spread, most, cuts=(), kind=jnp.bfloat16):
    entries = spread * jax.random.normal(own_key, shape, jnp.float32)
    if cuts:
        entries = entries * block_levels(own_key, shape, cuts, -0.22, 0.18)
    return jnp.clip(entries, -most, most).astype(kind)


def setup_inputs(seed: int = 0) -> dict:
    splits = jax.random.split(jax.random.key(seed), 8)
    return {
        "queries": draw_queries(jax.random.fold_in(splits[7], 71), 0),
        "keys": centred(splits[1], (TOKENS, HK * DH), 1.0, 6.0, ((0, 32),)),
        "values": centred(splits[2], (TOKENS, HK * DH), 1.0, 6.0, ((0, 32),)),
        "mid_key_weight": centred(splits[3], (MID * DH, DH), (MID * DH) ** -0.5, 0.1875),
        "mid_value_weight": centred(splits[4], (MID * DH, DH), (MID * DH) ** -0.5, 0.1875),
        "far_key_weight": centred(splits[5], (FAR * DH, DH), (FAR * DH) ** -0.5, 0.125),
        "far_value_weight": centred(splits[6], (FAR * DH, DH), (FAR * DH) ** -0.5, 0.125),
    }


NEG_FILL = -1e30


def squeeze_groups(source, weight, squeeze):
    group_count = source.shape[0] // squeeze
    grouped = source.reshape(group_count, squeeze, HK, DH).transpose(0, 2, 1, 3).reshape(group_count, HK, squeeze * DH)
    merged = jnp.einsum("nhr,rd->nhd", grouped.astype(jnp.float32), weight.astype(jnp.float32))
    return merged.astype(jnp.bfloat16).reshape(group_count, HK * DH)


def attend(queries, keys, values, visible):
    group_size = HQ // HK
    query_rows = queries.shape[0]
    query4 = queries.reshape(query_rows, HK, group_size, DH).astype(jnp.float32)
    key_heads = keys.reshape(keys.shape[0], HK, DH).astype(jnp.float32)
    value_heads = values.reshape(values.shape[0], HK, DH).astype(jnp.float32)
    scores = jnp.einsum("thgd,shd->hgts", query4, key_heads) * (DH ** -0.5)
    top_score = jnp.max(jnp.where(visible, scores, NEG_FILL), axis=-1, keepdims=True)
    weights = jnp.exp(jnp.where(visible, scores - top_score, NEG_FILL))
    weight_sum = jnp.sum(weights, axis=-1)
    rounded = lax.optimization_barrier(weights.astype(jnp.bfloat16))
    mixed_out = jnp.einsum("hgts,shd->thgd", rounded.astype(jnp.float32), value_heads)
    weight_sum = jnp.transpose(weight_sum, (2, 0, 1))[..., None]
    return (mixed_out / jnp.maximum(weight_sum, 1.0)).reshape(query_rows, HQ * DH)


def reference(queries, keys, values, mid_key_weight, mid_value_weight, far_key_weight, far_value_weight):
    tok_rows = TOK_DEV
    mid_keys = squeeze_groups(keys, mid_key_weight, MID)
    mid_values = squeeze_groups(values, mid_value_weight, MID)
    far_keys = squeeze_groups(keys, far_key_weight, FAR)
    far_values = squeeze_groups(values, far_value_weight, FAR)
    row_mid = N_COL * tok_rows // MID
    row_far = N_COL * tok_rows // FAR
    zero_rows = jnp.zeros((3 * tok_rows, HK * DH), keys.dtype)
    padded_keys = jnp.concatenate([zero_rows, keys], axis=0)
    padded_values = jnp.concatenate([zero_rows, values], axis=0)
    far_row = jnp.arange(N_ROW * row_far, dtype=jnp.int32) // row_far

    def one_tile(device_pos):
        first_pos = device_pos * tok_rows
        query_pos = first_pos + jnp.arange(tok_rows, dtype=jnp.int32)
        query_tile = lax.dynamic_slice_in_dim(queries, first_pos, tok_rows, 0)
        near_keys = lax.dynamic_slice_in_dim(padded_keys, first_pos, 4 * tok_rows, 0)
        near_values = lax.dynamic_slice_in_dim(padded_values, first_pos, 4 * tok_rows, 0)
        key_pos = first_pos - 3 * tok_rows + jnp.arange(4 * tok_rows, dtype=jnp.int32)
        near_seen = (key_pos[None, :] <= query_pos[:, None]) & (key_pos[None, :] >= 0) & (key_pos[None, :] // BLOCK >= query_pos[:, None] // BLOCK - 1)
        grid_row = device_pos // N_COL
        row_first = grid_row * (N_COL * tok_rows)
        mid_k = lax.dynamic_slice_in_dim(mid_keys, grid_row * row_mid, row_mid, 0)
        mid_v = lax.dynamic_slice_in_dim(mid_values, grid_row * row_mid, row_mid, 0)
        mid_end = row_first + MID * jnp.arange(row_mid, dtype=jnp.int32) + MID - 1
        mid_seen = mid_end[None, :] <= query_pos[:, None]
        far_seen = jnp.broadcast_to(far_row[None, :] < grid_row, (tok_rows, N_ROW * row_far))
        summed = attend(query_tile, near_keys, near_values, near_seen)
        summed = summed + attend(query_tile, mid_k, mid_v, mid_seen)
        summed = summed + attend(query_tile, far_keys, far_values, far_seen)
        return summed.astype(jnp.bfloat16)

    all_tiles = lax.map(one_tile, jnp.arange(DEVICES, dtype=jnp.int32))
    return all_tiles.reshape(DEVICES * tok_rows, HQ * DH)
```

```python
import functools
import math

import jax
import jax.numpy as jnp
from jax import lax
from jax.experimental import pallas as pl
from jax.experimental.pallas import tpu as pltpu
from jax.sharding import PartitionSpec as P

HQ = 16
HK = 4
DH = 128
BLOCK = 512
MID = 8
FAR = 16
GROUP = HQ // HK
KV = HK * DH
NEG_FILL = -1e30
TOP_FLOOR = -1e29
SUM_ROWS = 16
EXP_SCALE = DH ** (-0.5) * math.log2(math.e)
FAR_CHUNK = 512
VMEM_LIMIT = 57 * 1024 * 1024
MESH = pl.DeviceIdType.MESH
FROM_PARTNER, FROM_BEHIND, RELAYED = 0, 1, 2


def score(k, q):
    return lax.dot_general(k, q, (((1,), (1,)), ((), ())), preferred_element_type=jnp.float32)


def powers(s, top):
    return jnp.exp2((s - top) * EXP_SCALE)


def top_of(parts):
    return functools.reduce(jnp.maximum, [jnp.max(s, axis=0, keepdims=True) for s in parts])


def flat(v):
    return jnp.concatenate([v.T, jnp.ones((SUM_ROWS, v.shape[0]), v.dtype)], axis=0)


def weigh(parts, top, flats):
    terms = [
        jnp.dot(v, powers(s, top).astype(jnp.bfloat16), preferred_element_type=jnp.float32)
        for s, v in zip(parts, flats)
    ]
    both = functools.reduce(jnp.add, terms)
    return both[DH:DH + 1], both[:DH]


def inverse(den):
    return 1.0 / jnp.maximum(den, 1.0)


def kernel(
    rows, cols,
    q_hbm, k_hbm, v_hbm, wmk_hbm, wmv_hbm, wfk_hbm, wfv_hbm, out_ref,
    q_ref, k_ref, v_ref, wmk_ref, wmv_ref, wfk_ref, wfv_ref, fetch_sem,
    wide, mid_buf, far_buf, near, top_ref, den_ref, acc_ref, rest_ref,
    near_send, near_recv, mid_send, mid_recv, pass_send, pass_recv,
    swap_send, swap_recv, side_send, side_recv,
    down_send, down_recv, cross_send, cross_recv, twin_send, twin_recv,
):
    tok = q_ref.shape[0]
    mids, fars = tok // MID, tok // FAR
    total = rows * cols
    pairs = cols // 2
    row, col = lax.axis_index("row"), lax.axis_index("col")
    pos = row * cols + col
    side = lax.rem(col, 2)
    pair = col // 2
    low = lax.rem(row, 2)
    high = row // 2
    other_row = row + 1 - 2 * low
    partner = (row, col + 1 - 2 * side)
    beside = (other_row, col)
    is_leaf = (low == 0) & (pair == 0)
    is_last = high + 1 == rows // 2

    def fetch(i, src, dst):
        return pltpu.make_async_copy(src, dst, fetch_sem.at[i])

    fetches = [
        fetch(i, src, dst)
        for i, (src, dst) in enumerate((
            (k_hbm, k_ref), (wfk_hbm, wfk_ref), (wmk_hbm, wmk_ref),
            (v_hbm, v_ref), (wfv_hbm, wfv_ref), (wmv_hbm, wmv_ref), (q_hbm, q_ref),
        ))
    ]
    for copy in fetches:
        copy.start()

    def loop(low, high, f):
        def step(i, _):
            f(i)
            return 0

        lax.fori_loop(low, high, step, 0)

    def at(linear):
        return (linear // cols, lax.rem(linear, cols))

    ahead = at(lax.rem(pos + 2, total))

    mid_buf[...] = jnp.zeros_like(mid_buf)

    def clear(c):
        far_buf[c] = jnp.zeros(far_buf.shape[1:], far_buf.dtype)

    loop(0, 2 * rows, clear)

    barrier = pltpu.get_barrier_semaphore()

    def greet(device):
        pl.semaphore_signal(barrier, inc=1, device_id=device, device_id_type=MESH)

    loop(1, cols, lambda i: greet((row, lax.rem(col + i, cols))))
    loop(0, pairs, lambda p: greet((other_row, 2 * p + side)))

    def greet_if(condition, device):
        @pl.when(condition)
        def _():
            greet(device)

        return condition.astype(jnp.int32)

    greeted = (
        cols - 1 + pairs
        + greet_if(jnp.logical_not(is_last), (row + 2, col))
        + greet_if(high > 0, (row - 2, col))
        + greet_if(pos + 2 < total, at(pos + 2))
        + greet_if(pos >= 2, at(pos - 2))
    )

    def head_lanes(h, base=0):
        return pl.ds(pl.multiple_of(base + h * DH, DH), DH)

    def remote(src, dst, send, recv, device):
        return pltpu.make_async_remote_copy(
            src_ref=src, dst_ref=dst, send_sem=send, recv_sem=recv,
            device_id=device, device_id_type=MESH,
        )

    def same(ref, send, recv, device):
        return remote(ref, ref, send, recv, device)

    def far_block(r, p):
        return far_buf.at[2 * r + side, pl.ds(pl.multiple_of(p * fars, fars), fars), :]

    def swap(p_to, p_from):
        return same(far_block(row, p_from), swap_send.at[p_to], swap_recv.at[p_from], (row, 2 * p_to + side))

    def side_swap(r, p_to, p_from):
        return same(far_block(r, p_from), side_send.at[p_to], side_recv.at[p_from], (other_row, 2 * p_to + side))

    def down(r):
        return same(far_buf.at[2 * r + side], down_send.at[r], down_recv.at[r], (row + 2, col))

    def cross(r):
        return same(far_buf.at[2 * r + side], cross_send.at[r], cross_recv.at[r], beside)

    def twin(r, s):
        return same(far_buf.at[2 * r + s], twin_send.at[r], twin_recv.at[r], partner)

    def mid_span(c):
        return mid_buf.at[pl.ds(pl.multiple_of(c * mids, mids), mids), :]

    def mid_copy(p_to, p_from):
        return same(mid_span(2 * p_from + side), mid_send.at[p_to], mid_recv.at[p_from], (row, 2 * p_to + side))

    def mid_pass(p, s):
        return same(mid_span(2 * p + s), pass_send.at[p], pass_recv.at[p], partner)

    def near_copy(i):
        return remote(
            own[i], near.at[FROM_PARTNER, i], near_send.at[FROM_PARTNER, i, 0],
            near_recv.at[FROM_PARTNER, i, 0], partner,
        )

    def behind_copy(i, h):
        lanes = head_lanes(h)
        return remote(
            own[i].at[:, lanes], near.at[FROM_BEHIND, i, :, lanes],
            near_send.at[FROM_BEHIND, i, h], near_recv.at[FROM_BEHIND, i, h], ahead,
        )

    def relay_copy(i, h):
        lanes = head_lanes(h)
        return remote(
            near.at[FROM_BEHIND, i, :, lanes], near.at[RELAYED, i, :, lanes],
            near_send.at[RELAYED, i, h], near_recv.at[RELAYED, i, h], partner,
        )

    def behind_start(h):
        for i in range(2):
            behind_copy(i, h).start()

    own = (k_ref, v_ref)
    mid_rows = pl.ds(pl.multiple_of(col * mids, mids), mids)
    far_rows = pl.ds(pl.multiple_of(pair * fars, fars), fars)

    def summarise(s, src, wm, wf):
        for copy in fetches[3 * s:3 * s + 3]:
            copy.wait()
        for h in range(HK):
            wide[s * HK + h] = src[:, h * DH:(h + 1) * DH].astype(jnp.float32)
        for squeeze, count, weight in ((FAR, fars, wf), (MID, mids, wm)):
            grouped = jnp.concatenate(
                [
                    jnp.concatenate(
                        [wide[s * HK + h, pl.ds(i, count, stride=squeeze), :] for h in range(HK)],
                        axis=0,
                    ).astype(jnp.bfloat16)
                    for i in range(squeeze)
                ],
                axis=1,
            )
            merged = jnp.dot(grouped, weight[...], preferred_element_type=jnp.float32)
            merged = merged.astype(jnp.bfloat16)
            for h in range(HK):
                lanes = slice(s * KV + h * DH, s * KV + (h + 1) * DH)
                piece = merged[h * count:(h + 1) * count]
                if squeeze == FAR:
                    far_buf[2 * row + side, far_rows, lanes] = piece
                else:
                    mid_buf[mid_rows, lanes] = piece

    def others(f):
        def one(p):
            @pl.when(p != pair)
            def _():
                f(p)

        loop(0, pairs, one)

    def when(condition, f):
        @pl.when(condition)
        def _():
            f()

    def side_pairs(f):
        loop(low, pairs, f)

    summarise(0, k_ref, wmk_ref, wfk_ref)
    summarise(1, v_ref, wmv_ref, wfv_ref)
    pl.semaphore_wait(barrier, greeted)

    others(lambda p: swap(p, pair).start())
    side_pairs(lambda p: side_swap(row, p, pair).start())
    loop(pair + 1, pairs, lambda p: mid_copy(p, pair).start())

    when(pos + 2 < total, lambda: behind_start(0))

    @pl.when(side == 0)
    def _():
        for i in range(2):
            near_copy(i).start()
        mid_pass(pair, 0).start()

    fetches[6].wait()

    def iota(shape, axis):
        return lax.broadcasted_iota(jnp.int32, shape, axis)

    def query(h, g):
        return q_ref[:, pl.ds(pl.multiple_of((h * GROUP + g) * DH, DH), DH)]

    def near_first(with_partner):
        def two(i):
            seen = iota((tok, tok), 0) <= iota((tok, tok), 1)
            work = []
            for h in (2 * i, 2 * i + 1):
                keys = [k_ref[:, head_lanes(h)]]
                flats = [flat(v_ref[:, head_lanes(h)])]
                if with_partner:
                    keys.append(near[FROM_PARTNER, 0, :, head_lanes(h)])
                    flats.append(flat(near[FROM_PARTNER, 1, :, head_lanes(h)]))
                for g in range(GROUP):
                    work.append((h * GROUP + g, [score(k, query(h, g)) for k in keys], flats))
            for n, parts, flats in work:
                parts = [jnp.where(seen, parts[0], NEG_FILL)] + parts[1:]
                top = top_of(parts)
                top_ref[n] = top
                den_ref[n], acc_ref[n] = weigh(parts, top, flats)

        return two

    def spread():
        others(lambda p: swap(p, p).wait_recv())

        @pl.when(jnp.logical_not(is_leaf))
        def _():
            loop(0, pairs, lambda p: side_swap(other_row, p, p).wait_recv())

            @pl.when(jnp.logical_not(is_last))
            def _():
                loop(0, 2, lambda i: down(2 * high + i).start())

        when(low == 1, lambda: twin(row - 1, side).start())
        when(pos + 2 < total, lambda: loop(1, HK, behind_start))

    def near_own(with_partner):
        two = near_first(with_partner)

        def step(i):
            two(i)
            when(i == 0, spread)

        loop(0, HK // 2, step)

    @pl.when(side == 0)
    def _():
        near_own(False)

    @pl.when(side == 1)
    def _():
        for i in range(2):
            near_copy(i).wait_recv()
        near_own(True)

    def mid_arrive(p):
        mid_copy(p, p).wait_recv()
        mid_pass(p, side).start()

    loop(0, pair, mid_arrive)
    loop(0, pair, lambda p: mid_pass(p, 1 - side).wait_recv())

    @pl.when(side == 1)
    def _():
        mid_pass(pair, 0).wait_recv()

    n_mid = mid_buf.shape[0]

    def mid_two(i):
        seen = (iota((n_mid, tok), 0) * MID + MID - 1) <= (iota((n_mid, tok), 1) + col * tok)
        work = []
        for h in (2 * i, 2 * i + 1):
            keys = mid_buf[:, head_lanes(h)]
            values = flat(mid_buf[:, head_lanes(h, KV)])
            for g in range(GROUP):
                work.append((h * GROUP + g, score(keys, query(h, g)), values))
        for n, s, values in work:
            s = jnp.where(seen, s, NEG_FILL)
            den, acc = weigh([s], jnp.maximum(top_of([s]), TOP_FLOOR), [values])
            rest_ref[n] = acc * inverse(den)

    loop(0, HK // 2, mid_two)

    def hand_on(k):
        def one(i):
            r = 2 * (high - 1 - k) + i

            @pl.when(is_leaf)
            def _():
                cross(r).wait_recv()

            @pl.when(jnp.logical_not(is_leaf))
            def _():
                down(r).wait_recv()
                when(jnp.logical_not(is_last), lambda: down(r).start())
                when((low == 1) & (pair == 0), lambda: cross(r).start())

            twin(r, side).start()

        loop(0, 2, one)

    def arrive(h):
        for i in range(2):
            behind_copy(i, h).wait_recv()
            relay_copy(i, h).start()

    def near_last(h):
        for i in range(2):
            relay_copy(i, h).wait_recv()
        slots = (FROM_BEHIND, RELAYED)
        keys = [near[slot, 0, :, head_lanes(h)] for slot in slots]
        flats = [flat(near[slot, 1, :, head_lanes(h)]) for slot in slots]
        work = [[score(k, query(h, g)) for k in keys] for g in range(GROUP)]
        for g, parts in enumerate(work):
            n = h * GROUP + g
            before = top_ref[n]
            top = jnp.maximum(before, top_of(parts))
            den, acc = weigh(parts, top, flats)
            fade = powers(before, top)
            den_ref[n] = den_ref[n] * fade + den
            acc_ref[n] = acc_ref[n] * fade + acc

    line = far_buf.shape[1]
    per = max(1, min(2 * rows, FAR_CHUNK // line))
    n_chunk = 2 * rows // per

    def far_two(i):
        def part(h, j, base):
            block = far_buf[pl.ds(j * per, per), :, head_lanes(h, base)]
            return block.reshape(per * line, DH)

        def chunk(j, carry):
            seen = iota((per * line, 1), 0) + j * (per * line) < 2 * row * line
            work = []
            for h in (2 * i, 2 * i + 1):
                keys, flats = part(h, j, 0), flat(part(h, j, KV))
                work += [(score(keys, query(h, g)), flats) for g in range(GROUP)]
            after = []
            for m, (s, flats) in enumerate(work):
                s = jnp.where(seen, s, NEG_FILL)
                top = top_of([s])
                if carry is None:
                    after.append((top, *weigh([s], top, [flats])))
                    continue
                before, den, acc = carry[m]
                top = jnp.maximum(before, top)
                fade = powers(before, top)
                more, extra = weigh([s], top, [flats])
                after.append((top, den * fade + more, acc * fade + extra))
            return after

        carry = chunk(0, None)
        if n_chunk > 1:
            carry = lax.fori_loop(1, (2 * row + per - 1) // per, chunk, carry)
        for m, (_, den, acc) in enumerate(carry):
            n = 2 * i * GROUP + m
            rest_ref[n] = rest_ref[n] + acc * inverse(den)

    def finish(h):
        for g in range(GROUP):
            n = h * GROUP + g
            whole = acc_ref[n] * inverse(den_ref[n]) + rest_ref[n]
            lanes = pl.ds(pl.multiple_of(n * DH, DH), DH)
            out_ref[:, lanes] = whole.astype(out_ref.dtype).T

    def near_step(h):
        when(h < high, lambda: hand_on(h))

        @pl.when(pos >= 2)
        def _():
            arrive(h)
            near_last(h)

    loop(0, HK - 1, near_step)

    loop(HK - 1, high, hand_on)

    loop(0, row, lambda r: twin(r, 1 - side).wait_recv())

    @pl.when(pos >= 2)
    def _():
        arrive(HK - 1)

    @pl.when(row > 0)
    def _():
        loop(0, HK // 2, far_two)

    loop(0, HK - 1, finish)

    @pl.when(pos >= 2)
    def _():
        near_last(HK - 1)

    finish(HK - 1)

    others(lambda p: swap(p, pair).wait_send())
    loop(pair + 1, pairs, lambda p: mid_copy(p, pair).wait_send())
    side_pairs(lambda p: side_swap(row, p, pair).wait_send())

    @pl.when(jnp.logical_not(is_leaf) & jnp.logical_not(is_last))
    def _():
        loop(0, 2 * high + 2, lambda r: down(r).wait_send())

    @pl.when((low == 1) & (pair == 0))
    def _():
        loop(0, 2 * high, lambda r: cross(r).wait_send())

    loop(0, pair, lambda p: mid_pass(p, side).wait_send())
    loop(0, row, lambda r: twin(r, side).wait_send())

    @pl.when(side == 0)
    def _():
        for i in range(2):
            near_copy(i).wait_send()
        mid_pass(pair, 0).wait_send()

    @pl.when(pos + 2 < total)
    def _():
        for i in range(2):
            loop(0, HK, lambda h, i=i: behind_copy(i, h).wait_send())

    @pl.when(pos >= 2)
    def _():
        for i in range(2):
            loop(0, HK, lambda h, i=i: relay_copy(i, h).wait_send())


def body(rows, cols, queries, keys, values, *weights):
    tok = queries.shape[0]
    assert BLOCK == 2 * tok and cols % 2 == 0 and rows % 2 == 0
    dma = pltpu.SemaphoreType.DMA
    bf16, f32 = jnp.bfloat16, jnp.float32
    vmem = pl.BlockSpec(memory_space=pltpu.VMEM)
    pairs = cols // 2
    return pl.pallas_call(
        functools.partial(kernel, rows, cols),
        out_shape=pltpu.VMEM(queries.shape, bf16),
        in_specs=[pl.BlockSpec(memory_space=pltpu.HBM)] * 7,
        out_specs=vmem,
        scratch_shapes=[
            *[pltpu.VMEM(a.shape, a.dtype) for a in (queries, keys, values, *weights)],
            dma((7,)),
            pltpu.VMEM((2 * HK, tok, DH), f32),
            pltpu.VMEM((cols * (tok // MID), 2 * KV), bf16),
            pltpu.VMEM((2 * rows, pairs * (tok // FAR), 2 * KV), bf16),
            pltpu.VMEM((3, 2, tok, KV), bf16),
            pltpu.VMEM((HQ, 1, tok), f32),
            pltpu.VMEM((HQ, 1, tok), f32),
            pltpu.VMEM((HQ, DH, tok), f32),
            pltpu.VMEM((HQ, DH, tok), f32),
            dma((3, 2, HK)),
            dma((3, 2, HK)),
            *[dma((pairs,))] * 8,
            *[dma((rows,))] * 6,
        ],
        compiler_params=pltpu.CompilerParams(
            collective_id=0, has_side_effects=True, vmem_limit_bytes=VMEM_LIMIT
        ),
    )(queries, keys, values, *weights)


def solution(mesh):
    spec = P(("row", "col"), None)
    return jax.shard_map(
        functools.partial(body, mesh.shape["row"], mesh.shape["col"]),
        mesh=mesh,
        in_specs=(spec, spec, spec, P(), P(), P(), P()),
        out_specs=spec,
        check_vma=False,
    )
```

```python
import functools
import math

import jax
import jax.numpy as jnp
from jax import lax
from jax.experimental import pallas as pl
from jax.experimental.pallas import tpu as pltpu
from jax.sharding import PartitionSpec as P

HQ = 16
HK = 4
DH = 128
BLOCK = 512
MID = 8
FAR = 16
GROUP = HQ // HK
KV = HK * DH
NEG_FILL = -1e30
TOP_FLOOR = -1e29
SUM_ROWS = 16
EXP_SCALE = DH ** (-0.5) * math.log2(math.e)
FAR_CHUNK = 256
VMEM_LIMIT = 57 * 1024 * 1024
MESH = pl.DeviceIdType.MESH
FROM_PARTNER, FROM_BEHIND, RELAYED = 0, 1, 2


def score(k, q):
    return lax.dot_general(k, q, (((1,), (1,)), ((), ())), preferred_element_type=jnp.float32)


def powers(s, top):
    return jnp.exp2((s - top) * EXP_SCALE)


def top_of(parts):
    return functools.reduce(jnp.maximum, [jnp.max(s, axis=0, keepdims=True) for s in parts])


def flat(v):
    return jnp.concatenate([v.T, jnp.ones((SUM_ROWS, v.shape[0]), v.dtype)], axis=0)


def weigh(parts, top, flats):
    terms = [
        jnp.dot(v, powers(s, top).astype(jnp.bfloat16), preferred_element_type=jnp.float32)
        for s, v in zip(parts, flats)
    ]
    both = functools.reduce(jnp.add, terms)
    return both[DH:DH + 1], both[:DH]


def inverse(den):
    return 1.0 / jnp.maximum(den, 1.0)


def kernel(
    rows, cols,
    q_hbm, k_hbm, v_hbm, wmk_hbm, wmv_hbm, wfk_hbm, wfv_hbm, out_ref,
    q_ref, k_ref, v_ref, wmk_ref, wmv_ref, wfk_ref, wfv_ref, fetch_sem,
    wide, mid_buf, far_buf, near, top_ref, den_ref, acc_ref, rest_ref,
    far_top, far_den, far_acc,
    near_send, near_recv, mid_send, mid_recv, pass_send, pass_recv,
    swap_send, swap_recv, side_send, side_recv,
    down_send, down_recv, cross_send, cross_recv, lift_send, lift_recv, twin_send, twin_recv,
):
    tok = q_ref.shape[0]
    mids, fars = tok // MID, tok // FAR
    total = rows * cols
    pairs = cols // 2
    row, col = lax.axis_index("row"), lax.axis_index("col")
    pos = row * cols + col
    side = lax.rem(col, 2)
    pair = col // 2
    low = lax.rem(row, 2)
    high = row // 2
    other_row = row + 1 - 2 * low
    partner = (row, col + 1 - 2 * side)
    beside = (other_row, col)
    is_hub = (low == 1) & (pair == pairs - 1)
    feeds_beside = (low == 0) & (pair == pairs - 1)
    feeds_next = (low == 1) & (pair == pairs - 2)
    is_last = high + 1 == rows // 2

    def fetch(i, src, dst):
        return pltpu.make_async_copy(src, dst, fetch_sem.at[i])

    fetches = [
        fetch(i, src, dst)
        for i, (src, dst) in enumerate((
            (k_hbm, k_ref), (v_hbm, v_ref), (wfk_hbm, wfk_ref), (wfv_hbm, wfv_ref),
            (wmk_hbm, wmk_ref), (wmv_hbm, wmv_ref), (q_hbm, q_ref),
        ))
    ]
    for copy in fetches:
        copy.start()

    def loop(low, high, f):
        def step(i, _):
            f(i)
            return 0

        lax.fori_loop(low, high, step, 0)

    def at(linear):
        return (linear // cols, lax.rem(linear, cols))

    ahead = at(lax.rem(pos + 2, total))

    mid_buf[...] = jnp.zeros_like(mid_buf)

    far_top[...] = jnp.full_like(far_top, TOP_FLOOR)
    far_den[...] = jnp.zeros_like(far_den)

    def reset(n):
        far_acc[n] = jnp.zeros(far_acc.shape[1:], far_acc.dtype)

    loop(0, HQ, reset)

    def clear(c):
        far_buf[c] = jnp.zeros(far_buf.shape[1:], far_buf.dtype)

    loop(0, 2 * rows, clear)

    barrier = pltpu.get_barrier_semaphore()

    def greet(device):
        pl.semaphore_signal(barrier, inc=1, device_id=device, device_id_type=MESH)

    loop(1, cols, lambda i: greet((row, lax.rem(col + i, cols))))
    loop(0, pairs, lambda p: greet((other_row, 2 * p + side)))

    def greet_if(condition, device):
        @pl.when(condition)
        def _():
            greet(device)

        return condition.astype(jnp.int32)

    greeted = (
        cols - 1 + pairs
        + greet_if(jnp.logical_not(is_last), (row + 2, col))
        + greet_if(high > 0, (row - 2, col))
        + greet_if(pos + 2 < total, at(pos + 2))
        + greet_if(pos >= 2, at(pos - 2))
    )

    def head_lanes(h, base=0):
        return pl.ds(pl.multiple_of(base + h * DH, DH), DH)

    def remote(src, dst, send, recv, device):
        return pltpu.make_async_remote_copy(
            src_ref=src, dst_ref=dst, send_sem=send, recv_sem=recv,
            device_id=device, device_id_type=MESH,
        )

    def same(ref, send, recv, device):
        return remote(ref, ref, send, recv, device)

    def far_block(r, p):
        return far_buf.at[2 * r + side, pl.ds(pl.multiple_of(p * fars, fars), fars), :]

    def swap(p_to, p_from):
        return same(far_block(row, p_from), swap_send.at[p_to], swap_recv.at[p_from], (row, 2 * p_to + side))

    def side_swap(r, p_to, p_from):
        return same(far_block(r, p_from), side_send.at[p_to], side_recv.at[p_from], (other_row, 2 * p_to + side))

    def down(r):
        return same(far_buf.at[2 * r + side], down_send.at[r], down_recv.at[r], (row + 2, col))

    def cross(r):
        return same(far_buf.at[2 * r + side], cross_send.at[r], cross_recv.at[r], beside)

    def lift(r):
        return same(far_buf.at[2 * r + side], lift_send.at[r], lift_recv.at[r], (row, col + 2))

    def twin(r, s):
        return same(far_buf.at[2 * r + s], twin_send.at[r], twin_recv.at[r], partner)

    def mid_span(c):
        return mid_buf.at[pl.ds(pl.multiple_of(c * mids, mids), mids), :]

    def mid_copy(p_to, p_from):
        return same(mid_span(2 * p_from + side), mid_send.at[p_to], mid_recv.at[p_from], (row, 2 * p_to + side))

    def mid_pass(p, s):
        return same(mid_span(2 * p + s), pass_send.at[p], pass_recv.at[p], partner)

    def near_copy(i, half):
        lanes = pl.ds(pl.multiple_of(half * (KV // 2), KV // 2), KV // 2)
        return remote(
            own[i].at[:, lanes], near.at[FROM_PARTNER, i, :, lanes],
            near_send.at[FROM_PARTNER, i, half], near_recv.at[FROM_PARTNER, i, half], partner,
        )

    def halves(f):
        for half in range(2):
            for i in range(2):
                f(near_copy(i, half))

    def behind_copy(i, h):
        lanes = head_lanes(h)
        return remote(
            own[i].at[:, lanes], near.at[FROM_BEHIND, i, :, lanes],
            near_send.at[FROM_BEHIND, i, h], near_recv.at[FROM_BEHIND, i, h], ahead,
        )

    def relay_copy(i, h):
        lanes = head_lanes(h)
        return remote(
            near.at[FROM_BEHIND, i, :, lanes], near.at[RELAYED, i, :, lanes],
            near_send.at[RELAYED, i, h], near_recv.at[RELAYED, i, h], partner,
        )

    def behind_start(h):
        for i in range(2):
            behind_copy(i, h).start()

    own = (k_ref, v_ref)
    mid_rows = pl.ds(pl.multiple_of(col * mids, mids), mids)
    far_rows = pl.ds(pl.multiple_of(pair * fars, fars), fars)

    def spread_out(s, src):
        for h in range(HK):
            wide[s * HK + h] = src[:, h * DH:(h + 1) * DH].astype(jnp.float32)

    def summarise(s, squeeze, weight):
        count = tok // squeeze
        grouped = jnp.concatenate(
            [
                jnp.concatenate(
                    [wide[s * HK + h, pl.ds(i, count, stride=squeeze), :] for h in range(HK)],
                    axis=0,
                ).astype(jnp.bfloat16)
                for i in range(squeeze)
            ],
            axis=1,
        )
        merged = jnp.dot(grouped, weight[...], preferred_element_type=jnp.float32)
        merged = merged.astype(jnp.bfloat16)
        for h in range(HK):
            lanes = slice(s * KV + h * DH, s * KV + (h + 1) * DH)
            piece = merged[h * count:(h + 1) * count]
            if squeeze == FAR:
                far_buf[2 * row + side, far_rows, lanes] = piece
            else:
                mid_buf[mid_rows, lanes] = piece

    def others(f):
        def one(p):
            @pl.when(p != pair)
            def _():
                f(p)

        loop(0, pairs, one)

    def when(condition, f):
        @pl.when(condition)
        def _():
            f()

    for copy in fetches[:2]:
        copy.wait()
    pl.semaphore_wait(barrier, greeted)
    when(side == 0, lambda: halves(lambda copy: copy.start()))
    spread_out(0, k_ref)
    spread_out(1, v_ref)
    for copy in fetches[2:4]:
        copy.wait()
    summarise(0, FAR, wfk_ref)
    summarise(1, FAR, wfv_ref)
    others(lambda p: swap(p, pair).start())
    loop(0, pairs, lambda p: side_swap(row, p, pair).start())
    for copy in fetches[4:6]:
        copy.wait()
    summarise(0, MID, wmk_ref)
    summarise(1, MID, wmv_ref)
    loop(pair + 1, pairs, lambda p: mid_copy(p, pair).start())
    when(side == 0, lambda: mid_pass(pair, 0).start())

    leads = pair == pairs - 1
    sends = pos + 2 < total
    when(feeds_beside & sends, lambda: behind_start(0))

    fetches[6].wait()

    def iota(shape, axis):
        return lax.broadcasted_iota(jnp.int32, shape, axis)

    def query(h, g):
        return q_ref[:, pl.ds(pl.multiple_of((h * GROUP + g) * DH, DH), DH)]

    def near_first(with_partner):
        def two(i):
            seen = iota((tok, tok), 0) <= iota((tok, tok), 1)
            work = []
            if with_partner:
                near_copy(0, i).wait_recv()
                near_copy(1, i).wait_recv()
            for h in (2 * i, 2 * i + 1):
                keys = [k_ref[:, head_lanes(h)]]
                flats = [flat(v_ref[:, head_lanes(h)])]
                if with_partner:
                    keys.append(near[FROM_PARTNER, 0, :, head_lanes(h)])
                    flats.append(flat(near[FROM_PARTNER, 1, :, head_lanes(h)]))
                for g in range(GROUP):
                    work.append((h * GROUP + g, [score(k, query(h, g)) for k in keys], flats))
            for n, parts, flats in work:
                parts = [jnp.where(seen, parts[0], NEG_FILL)] + parts[1:]
                top = top_of(parts)
                top_ref[n] = top
                den_ref[n], acc_ref[n] = weigh(parts, top, flats)

        return two

    def spread():
        others(lambda p: swap(p, p).wait_recv())
        others(lambda p: side_swap(other_row, p, p).wait_recv())
        when(jnp.logical_not(is_last), lambda: loop(0, 2, lambda i: down(2 * high + i).start()))
        when(leads & sends, lambda: loop(2, HK, behind_start))
        when(low == 1, lambda: twin(row - 1, side).start())

    def near_more():
        side_swap(other_row, pair, pair).wait_recv()
        when(sends, lambda: loop(jnp.where(feeds_beside, 1, 0), jnp.where(leads, 2, HK), behind_start))

    def near_own(with_partner):
        two = near_first(with_partner)

        def step(i):
            if with_partner:
                when(i == 0, near_more)
            two(i)
            if with_partner:
                when(i == 0, spread)
            else:
                when(i == 0, near_more)
                when(i == 1, spread)

        loop(0, HK // 2, step)

    @pl.when(side == 0)
    def _():
        near_own(False)

    @pl.when(side == 1)
    def _():
        near_own(True)

    def mid_arrive(p):
        mid_copy(p, p).wait_recv()
        mid_pass(p, side).start()

    loop(0, pair, mid_arrive)
    loop(0, pair, lambda p: mid_pass(p, 1 - side).wait_recv())

    @pl.when(side == 1)
    def _():
        mid_pass(pair, 0).wait_recv()

    n_mid = mid_buf.shape[0]

    def mid_two(i):
        seen = (iota((n_mid, tok), 0) * MID + MID - 1) <= (iota((n_mid, tok), 1) + col * tok)
        work = []
        for h in (2 * i, 2 * i + 1):
            keys = mid_buf[:, head_lanes(h)]
            values = flat(mid_buf[:, head_lanes(h, KV)])
            for g in range(GROUP):
                work.append((h * GROUP + g, score(keys, query(h, g)), values))
        for n, s, values in work:
            s = jnp.where(seen, s, NEG_FILL)
            den, acc = weigh([s], jnp.maximum(top_of([s]), TOP_FLOOR), [values])
            rest_ref[n] = acc * inverse(den)

    loop(0, HK // 2, mid_two)

    def hand_on(k):
        def one(i):
            r = 2 * (high - 1 - k) + i

            @pl.when(is_hub)
            def _():
                when(k == 0, lambda: down(r).wait_recv())
                when(k == 1, lambda: cross(r).wait_recv())
                when(k > 1, lambda: lift(r).wait_recv())

            @pl.when(jnp.logical_not(is_hub))
            def _():
                down(r).wait_recv()
                when(jnp.logical_not(is_last), lambda: down(r).start())
                when(feeds_beside & (k == 1), lambda: cross(r).start())
                when(feeds_next & (k > 1), lambda: lift(r).start())

            twin(r, side).start()

        loop(0, 2, one)

    def arrive(h):
        for i in range(2):
            behind_copy(i, h).wait_recv()
            relay_copy(i, h).start()

    def near_last(h):
        for i in range(2):
            relay_copy(i, h).wait_recv()
        slots = (FROM_BEHIND, RELAYED)
        keys = [near[slot, 0, :, head_lanes(h)] for slot in slots]
        flats = [flat(near[slot, 1, :, head_lanes(h)]) for slot in slots]
        work = [[score(k, query(h, g)) for k in keys] for g in range(GROUP)]
        for g, parts in enumerate(work):
            n = h * GROUP + g
            before = top_ref[n]
            top = jnp.maximum(before, top_of(parts))
            den, acc = weigh(parts, top, flats)
            fade = powers(before, top)
            den_ref[n] = den_ref[n] * fade + den
            acc_ref[n] = acc_ref[n] * fade + acc

    line = far_buf.shape[1]
    per = max(1, min(2 * rows, FAR_CHUNK // line))
    def far_two(j, i):
        def part(h, base):
            block = far_buf[pl.ds(j * per, per), :, head_lanes(h, base)]
            return block.reshape(per * line, DH)

        seen = iota((per * line, 1), 0) + j * (per * line) < 2 * row * line
        work = []
        for h in (2 * i, 2 * i + 1):
            keys, flats = part(h, 0), flat(part(h, KV))
            work += [(h * GROUP + g, score(keys, query(h, g)), flats) for g in range(GROUP)]
        for n, s, flats in work:
            s = jnp.where(seen, s, NEG_FILL)
            before = far_top[n]
            top = jnp.maximum(before, top_of([s]))
            fade = powers(before, top)
            den, acc = weigh([s], top, [flats])
            far_top[n] = top
            far_den[n] = far_den[n] * fade + den
            far_acc[n] = far_acc[n] * fade + acc

    row_span = per // 2
    newest = (row + row_span - 1) // row_span - 1

    def far_chunks(name, low_chunk, high_chunk):
        loop(low_chunk * row_span, jnp.minimum(high_chunk * row_span, row), lambda r: twin(r, 1 - side).wait_recv())
        loop(low_chunk, high_chunk, lambda j: loop(0, HK // 2, functools.partial(far_two, j)))

    early = jnp.logical_not(is_hub) | (newest * row_span >= 2 * high)

    def finish(with_far, h):
        for g in range(GROUP):
            n = h * GROUP + g
            whole = acc_ref[n] * inverse(den_ref[n]) + rest_ref[n]
            if with_far:
                whole = whole + far_acc[n] * inverse(far_den[n])
            lanes = pl.ds(pl.multiple_of(n * DH, DH), DH)
            out_ref[:, lanes] = whole.astype(out_ref.dtype).T

    def near_in(h):
        when(pos >= 2, lambda: arrive(h))

    def near_step(h):
        when((h < high) & jnp.logical_not(is_hub), lambda: hand_on(h))
        near_in(h)
        when((h == 1) & (row > 0) & early, lambda: far_chunks("FAR1", newest, newest + 1))

        @pl.when(pos >= 2)
        def _():
            near_last(h)

    loop(0, HK - 1, near_step)

    @pl.when(is_hub & (high > 0))
    def _():
        hand_on(0)
        when(jnp.logical_not(early), lambda: far_chunks("FAR3", newest, newest + 1))

    loop(jnp.where(is_hub, 1, HK - 1), high, hand_on)
    near_in(HK - 1)

    @pl.when(row > 0)
    def _():
        far_chunks("FAR2", 0, newest)
        loop(0, HK - 1, functools.partial(finish, True))
        near_last(HK - 1)
        finish(True, HK - 1)

    @pl.when(row == 0)
    def _():
        @pl.when(pos >= 2)
        def _():
            near_last(HK - 1)

        loop(0, HK, functools.partial(finish, False))

    others(lambda p: swap(p, pair).wait_send())
    loop(pair + 1, pairs, lambda p: mid_copy(p, pair).wait_send())
    loop(0, pairs, lambda p: side_swap(row, p, pair).wait_send())

    loop(0, pair, lambda p: mid_pass(p, side).wait_send())

    @pl.when(jnp.logical_not(is_last))
    def _():
        loop(jnp.where(is_hub, 2 * high, 0), 2 * high + 2, lambda r: down(r).wait_send())

    @pl.when(feeds_beside & (high > 1))
    def _():
        loop(2 * high - 4, 2 * high - 2, lambda r: cross(r).wait_send())

    @pl.when(feeds_next)
    def _():
        loop(0, 2 * high - 4, lambda r: lift(r).wait_send())

    loop(0, row, lambda r: twin(r, side).wait_send())

    @pl.when(side == 0)
    def _():
        halves(lambda copy: copy.wait_send())
        mid_pass(pair, 0).wait_send()

    @pl.when(pos + 2 < total)
    def _():
        for i in range(2):
            loop(0, HK, lambda h, i=i: behind_copy(i, h).wait_send())

    @pl.when(pos >= 2)
    def _():
        for i in range(2):
            loop(0, HK, lambda h, i=i: relay_copy(i, h).wait_send())


def body(rows, cols, queries, keys, values, *weights):
    tok = queries.shape[0]
    assert BLOCK == 2 * tok and cols % 2 == 0 and rows % 2 == 0
    dma = pltpu.SemaphoreType.DMA
    bf16, f32 = jnp.bfloat16, jnp.float32
    vmem = pl.BlockSpec(memory_space=pltpu.VMEM)
    pairs = cols // 2
    return pl.pallas_call(
        functools.partial(kernel, rows, cols),
        out_shape=pltpu.VMEM(queries.shape, bf16),
        in_specs=[pl.BlockSpec(memory_space=pltpu.HBM)] * 7,
        out_specs=vmem,
        scratch_shapes=[
            *[pltpu.VMEM(a.shape, a.dtype) for a in (queries, keys, values, *weights)],
            dma((7,)),
            pltpu.VMEM((2 * HK, tok, DH), f32),
            pltpu.VMEM((cols * (tok // MID), 2 * KV), bf16),
            pltpu.VMEM((2 * rows, pairs * (tok // FAR), 2 * KV), bf16),
            pltpu.VMEM((3, 2, tok, KV), bf16),
            pltpu.VMEM((HQ, 1, tok), f32),
            pltpu.VMEM((HQ, 1, tok), f32),
            pltpu.VMEM((HQ, DH, tok), f32),
            pltpu.VMEM((HQ, DH, tok), f32),
            pltpu.VMEM((HQ, 1, tok), f32),
            pltpu.VMEM((HQ, 1, tok), f32),
            pltpu.VMEM((HQ, DH, tok), f32),
            dma((3, 2, HK)),
            dma((3, 2, HK)),
            *[dma((pairs,))] * 8,
            *[dma((rows,))] * 8,
        ],
        compiler_params=pltpu.CompilerParams(
            collective_id=0, has_side_effects=True, vmem_limit_bytes=VMEM_LIMIT
        ),
    )(queries, keys, values, *weights)


def solution(mesh):
    spec = P(("row", "col"), None)
    return jax.shard_map(
        functools.partial(body, mesh.shape["row"], mesh.shape["col"]),
        mesh=mesh,
        in_specs=(spec, spec, spec, P(), P(), P(), P()),
        out_specs=spec,
        check_vma=False,
    )
```

```python
import functools
import math

import jax
import jax.numpy as jnp
from jax import lax
from jax.experimental import pallas as pl
from jax.experimental.pallas import tpu as pltpu
from jax.sharding import PartitionSpec as P

HQ = 16
HK = 4
DH = 128
BLOCK = 512
MID = 8
FAR = 16
GROUP = HQ // HK
KV = HK * DH
NEG_FILL = -1e30
TOP_FLOOR = -1e29
SUM_ROWS = 16
N_FIRST = 2
EXP_SCALE = DH ** (-0.5) * math.log2(math.e)
FAR_CHUNK = 256
VMEM_LIMIT = 57 * 1024 * 1024
MESH = pl.DeviceIdType.MESH
FROM_PARTNER, FROM_BEHIND, RELAYED = 0, 1, 2


def score(k, q):
    return lax.dot_general(k, q, (((1,), (1,)), ((), ())), preferred_element_type=jnp.float32)


def powers(s, top):
    return jnp.exp2((s - top) * EXP_SCALE)


def top_of(parts):
    return functools.reduce(jnp.maximum, [jnp.max(s, axis=0, keepdims=True) for s in parts])


def flat(v):
    return jnp.concatenate([v.T, jnp.ones((SUM_ROWS, v.shape[0]), v.dtype)], axis=0)


def weigh(parts, top, flats):
    terms = [
        jnp.dot(v, powers(s, top).astype(jnp.bfloat16), preferred_element_type=jnp.float32)
        for s, v in zip(parts, flats)
    ]
    both = functools.reduce(jnp.add, terms)
    return both[DH:DH + 1], both[:DH]


def inverse(den):
    return 1.0 / jnp.maximum(den, 1.0)


def kernel(
    rows, cols,
    q_hbm, k_hbm, v_hbm, wmk_hbm, wmv_hbm, wfk_hbm, wfv_hbm, out_ref,
    q_ref, k_ref, v_ref, wmk_ref, wmv_ref, wfk_ref, wfv_ref, fetch_sem,
    wide, mid_buf, far_buf, near, top_ref, den_ref, acc_ref, rest_ref,
    far_top, far_den, far_acc,
    near_send, near_recv, mid_send, mid_recv, pass_send, pass_recv,
    swap_send, swap_recv, side_send, side_recv, up_send,
    down_send, down_recv, cross_send, cross_recv, lift_send, lift_recv, twin_send, twin_recv,
):
    tok = q_ref.shape[0]
    mids, fars = tok // MID, tok // FAR
    total = rows * cols
    pairs = cols // 2
    row, col = lax.axis_index("row"), lax.axis_index("col")
    pos = row * cols + col
    side = lax.rem(col, 2)
    pair = col // 2
    low = lax.rem(row, 2)
    high = row // 2
    other_row = row + 1 - 2 * low
    partner = (row, col + 1 - 2 * side)
    beside = (other_row, col)
    is_hub = (low == 1) & (pair == pairs - 1)
    feeds_beside = (low == 0) & (pair == pairs - 1)
    feeds_next = (low == 1) & (pair == pairs - 2)
    is_last = high + 1 == rows // 2

    def fetch(i, src, dst):
        return pltpu.make_async_copy(src, dst, fetch_sem.at[i])

    fetches = [
        fetch(i, src, dst)
        for i, (src, dst) in enumerate((
            (k_hbm, k_ref), (v_hbm, v_ref), (wfk_hbm, wfk_ref), (wfv_hbm, wfv_ref),
            (wmk_hbm, wmk_ref), (wmv_hbm, wmv_ref), (q_hbm, q_ref),
        ))
    ]
    for copy in fetches:
        copy.start()

    def loop(low, high, f):
        def step(i, _):
            f(i)
            return 0

        lax.fori_loop(low, high, step, 0)

    def at(linear):
        return (linear // cols, lax.rem(linear, cols))

    ahead = at(lax.rem(pos + 2, total))

    mid_buf[...] = jnp.zeros_like(mid_buf)

    far_top[...] = jnp.full_like(far_top, TOP_FLOOR)
    far_den[...] = jnp.zeros_like(far_den)

    def reset(n):
        far_acc[n] = jnp.zeros(far_acc.shape[1:], far_acc.dtype)

    loop(0, HQ, reset)

    def clear(c):
        far_buf[c] = jnp.zeros(far_buf.shape[1:], far_buf.dtype)

    loop(0, 2 * rows, clear)

    barrier = pltpu.get_barrier_semaphore()

    def greet(device):
        pl.semaphore_signal(barrier, inc=1, device_id=device, device_id_type=MESH)

    loop(1, cols, lambda i: greet((row, lax.rem(col + i, cols))))
    greet((other_row, col))

    def greet_if(condition, device):
        @pl.when(condition)
        def _():
            greet(device)

        return condition.astype(jnp.int32)

    greeted = (
        cols
        + greet_if(jnp.logical_not(is_last), (row + 2, col))
        + greet_if(high > 0, (row - 2, col))
        + greet_if(pos + 2 < total, at(pos + 2))
        + greet_if(pos >= 2, at(pos - 2))
    )

    def head_lanes(h, base=0):
        return pl.ds(pl.multiple_of(base + h * DH, DH), DH)

    def remote(src, dst, send, recv, device):
        return pltpu.make_async_remote_copy(
            src_ref=src, dst_ref=dst, send_sem=send, recv_sem=recv,
            device_id=device, device_id_type=MESH,
        )

    def same(ref, send, recv, device):
        return remote(ref, ref, send, recv, device)

    def far_block(r, p):
        return far_buf.at[2 * r + side, pl.ds(pl.multiple_of(p * fars, fars), fars), :]

    def swap(p_to, p_from):
        return same(far_block(row, p_from), swap_send.at[p_to], swap_recv.at[p_from], (row, 2 * p_to + side))

    def side_swap(r, p):
        return same(far_block(r, p), side_send.at[p], side_recv.at[p], beside)

    def up(p):
        return same(far_block(other_row, pair), up_send.at[p], side_recv.at[pair], (row, 2 * p + side))

    def down(r):
        return same(far_buf.at[2 * r + side], down_send.at[r], down_recv.at[r], (row + 2, col))

    def cross(r):
        return same(far_buf.at[2 * r + side], cross_send.at[r], cross_recv.at[r], beside)

    def lift(r):
        return same(far_buf.at[2 * r + side], lift_send.at[r], lift_recv.at[r], (row, col + 2))

    def twin(r, s):
        return same(far_buf.at[2 * r + s], twin_send.at[r], twin_recv.at[r], partner)

    def mid_span(c):
        return mid_buf.at[pl.ds(pl.multiple_of(c * mids, mids), mids), :]

    def mid_copy(p_to, p_from):
        return same(mid_span(2 * p_from + side), mid_send.at[p_to], mid_recv.at[p_from], (row, 2 * p_to + side))

    def mid_pass(p, s):
        return same(mid_span(2 * p + s), pass_send.at[p], pass_recv.at[p], partner)

    def near_copy(i, half):
        lanes = pl.ds(pl.multiple_of(half * (KV // 2), KV // 2), KV // 2)
        return remote(
            own[i].at[:, lanes], near.at[FROM_PARTNER, i, :, lanes],
            near_send.at[FROM_PARTNER, i, half], near_recv.at[FROM_PARTNER, i, half], partner,
        )

    def halves(f):
        for half in range(2):
            for i in range(2):
                f(near_copy(i, half))

    def behind_copy(i, h):
        lanes = head_lanes(h)
        return remote(
            own[i].at[:, lanes], near.at[FROM_BEHIND, i, :, lanes],
            near_send.at[FROM_BEHIND, i, h], near_recv.at[FROM_BEHIND, i, h], ahead,
        )

    def relay_copy(i, h):
        lanes = head_lanes(h)
        return remote(
            near.at[FROM_BEHIND, i, :, lanes], near.at[RELAYED, i, :, lanes],
            near_send.at[RELAYED, i, h], near_recv.at[RELAYED, i, h], partner,
        )

    def behind_start(h):
        for i in range(2):
            behind_copy(i, h).start()

    own = (k_ref, v_ref)
    mid_rows = pl.ds(pl.multiple_of(col * mids, mids), mids)
    far_rows = pl.ds(pl.multiple_of(pair * fars, fars), fars)

    def spread_out(s, src):
        for h in range(HK):
            wide[s * HK + h] = src[:, h * DH:(h + 1) * DH].astype(jnp.float32)

    def summarise(s, squeeze, weight):
        count = tok // squeeze
        grouped = jnp.concatenate(
            [
                jnp.concatenate(
                    [wide[s * HK + h, pl.ds(i, count, stride=squeeze), :] for h in range(HK)],
                    axis=0,
                ).astype(jnp.bfloat16)
                for i in range(squeeze)
            ],
            axis=1,
        )
        merged = jnp.dot(grouped, weight[...], preferred_element_type=jnp.float32)
        merged = merged.astype(jnp.bfloat16)
        for h in range(HK):
            lanes = slice(s * KV + h * DH, s * KV + (h + 1) * DH)
            piece = merged[h * count:(h + 1) * count]
            if squeeze == FAR:
                far_buf[2 * row + side, far_rows, lanes] = piece
            else:
                mid_buf[mid_rows, lanes] = piece

    def others(f):
        def one(p):
            @pl.when(p != pair)
            def _():
                f(p)

        loop(0, pairs, one)

    def when(condition, f):
        @pl.when(condition)
        def _():
            f()

    for copy in fetches[:2]:
        copy.wait()
    spread_out(0, k_ref)
    spread_out(1, v_ref)
    for copy in fetches[2:4]:
        copy.wait()
    summarise(0, FAR, wfk_ref)
    summarise(1, FAR, wfv_ref)
    pl.semaphore_wait(barrier, greeted)
    others(lambda p: swap(p, pair).start())
    side_swap(row, pair).start()
    when(side == 0, lambda: halves(lambda copy: copy.start()))
    for copy in fetches[4:6]:
        copy.wait()
    summarise(0, MID, wmk_ref)
    summarise(1, MID, wmv_ref)
    loop(pair + 1, pairs, lambda p: mid_copy(p, pair).start())
    when(side == 0, lambda: mid_pass(pair, 0).start())

    sends = pos + 2 < total
    n_first = jnp.where(is_hub, N_FIRST, HK)

    fetches[6].wait()

    def iota(shape, axis):
        return lax.broadcasted_iota(jnp.int32, shape, axis)

    def query(h, g):
        return q_ref[:, pl.ds(pl.multiple_of((h * GROUP + g) * DH, DH), DH)]

    def near_first(with_partner):
        def two(i):
            seen = iota((tok, tok), 0) <= iota((tok, tok), 1)
            work = []
            if with_partner:
                near_copy(0, i).wait_recv()
                near_copy(1, i).wait_recv()
            for h in (2 * i, 2 * i + 1):
                keys = [k_ref[:, head_lanes(h)]]
                flats = [flat(v_ref[:, head_lanes(h)])]
                if with_partner:
                    keys.append(near[FROM_PARTNER, 0, :, head_lanes(h)])
                    flats.append(flat(near[FROM_PARTNER, 1, :, head_lanes(h)]))
                for g in range(GROUP):
                    work.append((h * GROUP + g, [score(k, query(h, g)) for k in keys], flats))
            for n, parts, flats in work:
                parts = [jnp.where(seen, parts[0], NEG_FILL)] + parts[1:]
                top = top_of(parts)
                top_ref[n] = top
                den_ref[n], acc_ref[n] = weigh(parts, top, flats)

        return two

    def spread():
        others(lambda p: side_swap(other_row, p).wait_recv())
        when(jnp.logical_not(is_last), lambda: down(other_row).start())
        when(sends, lambda: loop(n_first, HK, behind_start))
        when(low == 1, lambda: twin(row - 1, side).start())

    def near_more():
        side_swap(other_row, pair).wait_recv()
        loop(pair + 1, pairs, lambda p: up(p).start())

        def over(p):
            swap(p, p).wait_recv()
            side_swap(row, p).start()

        loop(pair + 1, pairs, over)
        loop(0, pair, lambda p: swap(p, p).wait_recv())
        when(sends, lambda: loop(0, n_first, behind_start))
        when(jnp.logical_not(is_last), lambda: down(row).start())

    def near_own(with_partner):
        two = near_first(with_partner)

        def step(i):
            if with_partner:
                when(i == 0, near_more)
            two(i)
            if with_partner:
                when(i == 0, spread)
            else:
                when(i == 0, near_more)
                when(i == 1, spread)

        loop(0, HK // 2, step)

    @pl.when(side == 0)
    def _():
        near_own(False)

    @pl.when(side == 1)
    def _():
        near_own(True)

    def mid_arrive(p):
        mid_copy(p, p).wait_recv()
        mid_pass(p, side).start()

    loop(0, pair, mid_arrive)
    loop(0, pair, lambda p: mid_pass(p, 1 - side).wait_recv())

    @pl.when(side == 1)
    def _():
        mid_pass(pair, 0).wait_recv()

    n_mid = mid_buf.shape[0]

    def mid_all():
        seen = (iota((n_mid, tok), 0) * MID + MID - 1) <= (iota((n_mid, tok), 1) + col * tok)
        work = []
        for h in range(HK):
            keys = mid_buf[:, head_lanes(h)]
            values = flat(mid_buf[:, head_lanes(h, KV)])
            for g in range(GROUP):
                work.append((h * GROUP + g, score(keys, query(h, g)), values))
        for n, s, values in work:
            s = jnp.where(seen, s, NEG_FILL)
            den, acc = weigh([s], jnp.maximum(top_of([s]), TOP_FLOOR), [values])
            rest_ref[n] = acc * inverse(den)

    mid_all()

    def hand_on(k):
        def one(i):
            r = 2 * (high - 1 - k) + lax.rem(low + i, 2)

            @pl.when(is_hub)
            def _():
                when(k == 0, lambda: down(r).wait_recv())
                when(k == 1, lambda: cross(r).wait_recv())
                when(k > 1, lambda: lift(r).wait_recv())

            @pl.when(jnp.logical_not(is_hub))
            def _():
                down(r).wait_recv()
                when(jnp.logical_not(is_last), lambda: down(r).start())
                when(feeds_beside & (k == 1), lambda: cross(r).start())
                when(feeds_next & (k > 1), lambda: lift(r).start())

            twin(r, side).start()

        loop(0, 2, one)

    def arrive(h):
        for i in range(2):
            behind_copy(i, h).wait_recv()
            relay_copy(i, h).start()

    def near_last(h):
        for i in range(2):
            relay_copy(i, h).wait_recv()
        slots = (FROM_BEHIND, RELAYED)
        keys = [near[slot, 0, :, head_lanes(h)] for slot in slots]
        flats = [flat(near[slot, 1, :, head_lanes(h)]) for slot in slots]
        work = [[score(k, query(h, g)) for k in keys] for g in range(GROUP)]
        for g, parts in enumerate(work):
            n = h * GROUP + g
            before = top_ref[n]
            top = jnp.maximum(before, top_of(parts))
            den, acc = weigh(parts, top, flats)
            fade = powers(before, top)
            den_ref[n] = den_ref[n] * fade + den
            acc_ref[n] = acc_ref[n] * fade + acc

    line = far_buf.shape[1]
    per = max(1, min(2 * rows, FAR_CHUNK // line))
    def far_chunk(j):
        def part(h, base):
            block = far_buf[pl.ds(j * per, per), :, head_lanes(h, base)]
            return block.reshape(per * line, DH)

        seen = iota((per * line, 1), 0) + j * (per * line) < 2 * row * line
        work = []
        for h in range(HK):
            keys, flats = part(h, 0), flat(part(h, KV))
            work += [(h * GROUP + g, score(keys, query(h, g)), flats) for g in range(GROUP)]
        for n, s, flats in work:
            s = jnp.where(seen, s, NEG_FILL)
            before = far_top[n]
            top = jnp.maximum(before, top_of([s]))
            fade = powers(before, top)
            den, acc = weigh([s], top, [flats])
            far_top[n] = top
            far_den[n] = far_den[n] * fade + den
            far_acc[n] = far_acc[n] * fade + acc

    row_span = per // 2
    newest = (row + row_span - 1) // row_span - 1

    def far_chunks(name, low_chunk, high_chunk):
        loop(low_chunk * row_span, jnp.minimum(high_chunk * row_span, row), lambda r: twin(r, 1 - side).wait_recv())
        loop(low_chunk, high_chunk, far_chunk)

    def finish(with_far, h):
        for g in range(GROUP):
            n = h * GROUP + g
            whole = acc_ref[n] * inverse(den_ref[n]) + rest_ref[n]
            if with_far:
                whole = whole + far_acc[n] * inverse(far_den[n])
            lanes = pl.ds(pl.multiple_of(n * DH, DH), DH)
            out_ref[:, lanes] = whole.astype(out_ref.dtype).T

    def sent_early():
        others(lambda p: swap(p, pair).wait_send())
        loop(pair + 1, pairs, lambda p: mid_copy(p, pair).wait_send())
        loop(pair, pairs, lambda p: side_swap(row, p).wait_send())
        loop(pair + 1, pairs, lambda p: up(p).wait_send())
        loop(0, pair, lambda p: mid_pass(p, side).wait_send())

        @pl.when(side == 0)
        def _():
            halves(lambda copy: copy.wait_send())
            mid_pass(pair, 0).wait_send()

    def feeds_next_done():
        @pl.when(jnp.logical_not(is_last))
        def _():
            loop(jnp.where(is_hub, 2 * high, 0), 2 * high + 2, lambda r: down(r).wait_send())

        @pl.when(feeds_beside & (high > 1))
        def _():
            loop(2 * high - 4, 2 * high - 2, lambda r: cross(r).wait_send())

        @pl.when(feeds_next)
        def _():
            loop(0, 2 * high - 4, lambda r: lift(r).wait_send())

    def near_in(h):
        when(pos >= 2, lambda: arrive(h))

    def near_end(h):
        @pl.when(pos >= 2)
        def _():
            near_last(h)

    def far_newest():
        far_chunks("FAR1", newest, newest + 1)

    def far_rest():
        far_chunks("FAR2", 0, newest)

    plain = jnp.logical_not(is_hub)
    far_first = (low == 0) & (pair == 0)

    def step(s):
        when((s == 0) & (high > 0) & plain, lambda: hand_on(0))
        when((s < HK) & (s != 2), lambda: near_in(s))
        when((s == 1) & plain & (high > 1), lambda: hand_on(1))
        when(s > 0, lambda: near_end(s - 1))

        @pl.when(s == 2)
        def _():
            loop(jnp.where(is_hub, 0, 2), jnp.where(is_hub, jnp.minimum(high, 1), high), hand_on)

            def far(i):
                when((i == 0) != far_first, lambda: near_in(2))
                when((row > 0) & (i == 0), far_newest)

            loop(0, 2, far)
            when((row > 0) & plain, far_rest)

        @pl.when(s == HK - 1)
        def _():
            sent_early()
            when(is_hub, lambda: loop(1, high, hand_on))
            when(plain & (row > 0), lambda: loop(0, HK - 1, functools.partial(finish, True)))

    loop(0, HK + 1, step)

    @pl.when(row > 0)
    def _():
        when(is_hub, far_rest)
        loop(jnp.where(is_hub, 0, HK - 1), HK, functools.partial(finish, True))

    @pl.when(row == 0)
    def _():
        loop(0, HK, functools.partial(finish, False))

    loop(0, row, lambda r: twin(r, side).wait_send())
    feeds_next_done()

    @pl.when(pos + 2 < total)
    def _():
        for i in range(2):
            loop(0, HK, lambda h, i=i: behind_copy(i, h).wait_send())

    @pl.when(pos >= 2)
    def _():
        for i in range(2):
            loop(0, HK, lambda h, i=i: relay_copy(i, h).wait_send())


def body(rows, cols, queries, keys, values, *weights):
    tok = queries.shape[0]
    assert BLOCK == 2 * tok and cols % 2 == 0 and rows % 2 == 0
    dma = pltpu.SemaphoreType.DMA
    bf16, f32 = jnp.bfloat16, jnp.float32
    vmem = pl.BlockSpec(memory_space=pltpu.VMEM)
    pairs = cols // 2
    return pl.pallas_call(
        functools.partial(kernel, rows, cols),
        out_shape=pltpu.VMEM(queries.shape, bf16),
        in_specs=[pl.BlockSpec(memory_space=pltpu.HBM)] * 7,
        out_specs=vmem,
        scratch_shapes=[
            *[pltpu.VMEM(a.shape, a.dtype) for a in (queries, keys, values, *weights)],
            dma((7,)),
            pltpu.VMEM((2 * HK, tok, DH), f32),
            pltpu.VMEM((cols * (tok // MID), 2 * KV), bf16),
            pltpu.VMEM((2 * rows, pairs * (tok // FAR), 2 * KV), bf16),
            pltpu.VMEM((3, 2, tok, KV), bf16),
            pltpu.VMEM((HQ, 1, tok), f32),
            pltpu.VMEM((HQ, 1, tok), f32),
            pltpu.VMEM((HQ, DH, tok), f32),
            pltpu.VMEM((HQ, DH, tok), f32),
            pltpu.VMEM((HQ, 1, tok), f32),
            pltpu.VMEM((HQ, 1, tok), f32),
            pltpu.VMEM((HQ, DH, tok), f32),
            dma((3, 2, HK)),
            dma((3, 2, HK)),
            *[dma((pairs,))] * 9,
            *[dma((rows,))] * 8,
        ],
        compiler_params=pltpu.CompilerParams(
            collective_id=0, has_side_effects=True, vmem_limit_bytes=VMEM_LIMIT
        ),
    )(queries, keys, values, *weights)


def solution(mesh):
    spec = P(("row", "col"), None)
    return jax.shard_map(
        functools.partial(body, mesh.shape["row"], mesh.shape["col"]),
        mesh=mesh,
        in_specs=(spec, spec, spec, P(), P(), P(), P()),
        out_specs=spec,
        check_vma=False,
    )
```

```python
import functools
import math

import jax
import jax.numpy as jnp
from jax import lax
from jax.experimental import pallas as pl
from jax.experimental.pallas import tpu as pltpu
from jax.sharding import PartitionSpec as P

HQ = 16
HK = 4
DH = 128
BLOCK = 512
MID = 8
FAR = 16
GROUP = HQ // HK
KV = HK * DH
NEG_FILL = -1e30
TOP_FLOOR = -1e29
SUM_ROWS = 16
N_FIRST = 2
EXP_SCALE = DH ** (-0.5) * math.log2(math.e)
SLABS = 4
VMEM_LIMIT = 57 * 1024 * 1024
MESH = pl.DeviceIdType.MESH
FROM_PARTNER, FROM_BEHIND, RELAYED = 0, 1, 2


def score(k, q):
    return lax.dot_general(k, q, (((1,), (1,)), ((), ())), preferred_element_type=jnp.float32)


def powers(s, top):
    return jnp.exp2((s - top) * EXP_SCALE)


def top_of(parts):
    return functools.reduce(jnp.maximum, [jnp.max(s, axis=0, keepdims=True) for s in parts])


def flat(v):
    return jnp.concatenate([v.T, jnp.ones((SUM_ROWS, v.shape[0]), v.dtype)], axis=0)


def weigh(parts, top, flats):
    terms = [
        jnp.dot(v, powers(s, top).astype(jnp.bfloat16), preferred_element_type=jnp.float32)
        for s, v in zip(parts, flats)
    ]
    both = functools.reduce(jnp.add, terms)
    return both[DH:DH + 1], both[:DH]


def inverse(den):
    return 1.0 / jnp.maximum(den, 1.0)


def kernel(
    rows, cols,
    q_hbm, k_hbm, v_hbm, wmk_hbm, wmv_hbm, wfk_hbm, wfv_hbm, out_ref,
    q_ref, kv_ref, wmk_ref, wmv_ref, wfk_ref, wfv_ref, fetch_sem,
    wide, mid_buf, far_buf, near, top_ref, den_ref, acc_ref, rest_ref,
    far_top, far_den, far_acc,
    near_send, near_recv, mid_send, mid_recv, pass_send, pass_recv,
    swap_send, swap_recv, side_send, side_recv, up_send,
    down_send, down_recv, cross_send, cross_recv, lift_send, lift_recv, twin_send, twin_recv,
):
    tok = q_ref.shape[0]
    mids, fars = tok // MID, tok // FAR
    total = rows * cols
    pairs = cols // 2
    row, col = lax.axis_index("row"), lax.axis_index("col")
    pos = row * cols + col
    side = lax.rem(col, 2)
    pair = col // 2
    low = lax.rem(row, 2)
    high = row // 2
    other_row = row + 1 - 2 * low
    partner = (row, col + 1 - 2 * side)
    beside = (other_row, col)
    is_hub = (low == 1) & (pair == pairs - 1)
    feeds_beside = (low == 0) & (pair == pairs - 1)
    feeds_next = (low == 1) & (pair == pairs - 2)
    is_last = high + 1 == rows // 2

    def fetch(i, src, dst):
        return pltpu.make_async_copy(src, dst, fetch_sem.at[i])

    fetches = [
        fetch(i, src, dst)
        for i, (src, dst) in enumerate((
            (k_hbm, kv_ref.at[0]), (v_hbm, kv_ref.at[1]), (wfk_hbm, wfk_ref), (wfv_hbm, wfv_ref),
            (wmk_hbm, wmk_ref), (wmv_hbm, wmv_ref), (q_hbm, q_ref),
        ))
    ]
    for copy in fetches:
        copy.start()

    def loop(low, high, f):
        def step(i, _):
            f(i)
            return 0

        lax.fori_loop(low, high, step, 0)

    def at(linear):
        return (linear // cols, lax.rem(linear, cols))

    ahead = at(lax.rem(pos + 2, total))

    mid_buf[...] = jnp.zeros_like(mid_buf)

    far_top[...] = jnp.full_like(far_top, TOP_FLOOR)
    far_den[...] = jnp.zeros_like(far_den)

    def reset(n):
        far_acc[n] = jnp.zeros(far_acc.shape[1:], far_acc.dtype)

    loop(0, HQ, reset)

    def clear(c):
        far_buf[c] = jnp.zeros(far_buf.shape[1:], far_buf.dtype)

    loop(0, 2 * rows, clear)

    barrier = pltpu.get_barrier_semaphore()

    def greet(device):
        pl.semaphore_signal(barrier, inc=1, device_id=device, device_id_type=MESH)

    loop(1, cols, lambda i: greet((row, lax.rem(col + i, cols))))
    greet((other_row, col))

    def greet_if(condition, device):
        @pl.when(condition)
        def _():
            greet(device)

        return condition.astype(jnp.int32)

    greeted = (
        cols
        + greet_if(jnp.logical_not(is_last), (row + 2, col))
        + greet_if(high > 0, (row - 2, col))
        + greet_if(pos + 2 < total, at(pos + 2))
        + greet_if(pos >= 2, at(pos - 2))
    )

    def head_lanes(h, base=0):
        return pl.ds(pl.multiple_of(base + h * DH, DH), DH)

    def remote(src, dst, send, recv, device):
        return pltpu.make_async_remote_copy(
            src_ref=src, dst_ref=dst, send_sem=send, recv_sem=recv,
            device_id=device, device_id_type=MESH,
        )

    def same(ref, send, recv, device):
        return remote(ref, ref, send, recv, device)

    def far_block(r, p):
        return far_buf.at[2 * r + side, pl.ds(pl.multiple_of(p * fars, fars), fars), :]

    def swap(p_to, p_from):
        return same(far_block(row, p_from), swap_send.at[p_to], swap_recv.at[p_from], (row, 2 * p_to + side))

    def side_swap(r, p):
        return same(far_block(r, p), side_send.at[p], side_recv.at[p], beside)

    def up(p):
        return same(far_block(other_row, pair), up_send.at[p], side_recv.at[pair], (row, 2 * p + side))

    def down(r):
        return same(far_buf.at[2 * r + side], down_send.at[r], down_recv.at[r], (row + 2, col))

    def cross(r):
        return same(far_buf.at[2 * r + side], cross_send.at[lax.rem(r, 2)], cross_recv.at[lax.rem(r, 2)], beside)

    def lift(r):
        return same(far_buf.at[2 * r + side], lift_send.at[r], lift_recv.at[r], (row, col + 2))

    def twin(r, s):
        return same(far_buf.at[2 * r + s], twin_send.at[r], twin_recv.at[r], partner)

    def mid_span(c):
        return mid_buf.at[pl.ds(pl.multiple_of(c * mids, mids), mids), :]

    def mid_copy(p_to, p_from):
        return same(mid_span(2 * p_from + side), mid_send.at[p_to], mid_recv.at[p_from], (row, 2 * p_to + side))

    def mid_pass(p, s):
        return same(mid_span(2 * p + s), pass_send.at[p], pass_recv.at[p], partner)

    def near_copy(half):
        lanes = pl.ds(pl.multiple_of(half * (KV // 2), KV // 2), KV // 2)
        return remote(
            kv_ref.at[:, :, lanes], near.at[FROM_PARTNER, :, :, lanes],
            near_send.at[FROM_PARTNER, half], near_recv.at[FROM_PARTNER, half], partner,
        )

    def behind_copy(h):
        lanes = head_lanes(h)
        return remote(
            kv_ref.at[:, :, lanes], near.at[FROM_BEHIND, :, :, lanes],
            near_send.at[FROM_BEHIND, h], near_recv.at[FROM_BEHIND, h], ahead,
        )

    def relay_copy(h):
        lanes = head_lanes(h)
        return remote(
            near.at[FROM_BEHIND, :, :, lanes], near.at[RELAYED, :, :, lanes],
            near_send.at[RELAYED, h], near_recv.at[RELAYED, h], partner,
        )

    def behind_start(h):
        behind_copy(h).start()

    mid_rows = pl.ds(pl.multiple_of(col * mids, mids), mids)
    far_rows = pl.ds(pl.multiple_of(pair * fars, fars), fars)

    def spread_out(s):
        for h in range(HK):
            wide[s * HK + h] = kv_ref[s, :, h * DH:(h + 1) * DH].astype(jnp.float32)

    def summarise(s, squeeze, weight):
        count = tok // squeeze
        grouped = jnp.concatenate(
            [
                jnp.concatenate(
                    [wide[s * HK + h, pl.ds(i, count, stride=squeeze), :] for h in range(HK)],
                    axis=0,
                ).astype(jnp.bfloat16)
                for i in range(squeeze)
            ],
            axis=1,
        )
        merged = jnp.dot(grouped, weight[...], preferred_element_type=jnp.float32)
        merged = merged.astype(jnp.bfloat16)
        for h in range(HK):
            lanes = slice(s * KV + h * DH, s * KV + (h + 1) * DH)
            piece = merged[h * count:(h + 1) * count]
            if squeeze == FAR:
                far_buf[2 * row + side, far_rows, lanes] = piece
            else:
                mid_buf[mid_rows, lanes] = piece

    def others(f):
        def one(p):
            @pl.when(p != pair)
            def _():
                f(p)

        loop(0, pairs, one)

    def when(condition, f):
        @pl.when(condition)
        def _():
            f()

    for copy in fetches[:2]:
        copy.wait()
    spread_out(0)
    spread_out(1)
    for copy in fetches[2:4]:
        copy.wait()
    summarise(0, FAR, wfk_ref)
    summarise(1, FAR, wfv_ref)
    pl.semaphore_wait(barrier, greeted)
    others(lambda p: swap(p, pair).start())
    side_swap(row, pair).start()
    when(side == 0, lambda: loop(0, 2, lambda half: near_copy(half).start()))
    for copy in fetches[4:6]:
        copy.wait()
    summarise(0, MID, wmk_ref)
    summarise(1, MID, wmv_ref)
    loop(pair + 1, pairs, lambda p: mid_copy(p, pair).start())
    when(side == 0, lambda: mid_pass(pair, 0).start())

    sends = pos + 2 < total
    starts = feeds_beside & (side == 0)
    n_first = jnp.where(is_hub, N_FIRST, HK)

    fetches[6].wait()

    def iota(shape, axis):
        return lax.broadcasted_iota(jnp.int32, shape, axis)

    def query(h, g):
        return q_ref[:, pl.ds(pl.multiple_of((h * GROUP + g) * DH, DH), DH)]

    def near_first(with_partner):
        def two(i):
            seen = iota((tok, tok), 0) <= iota((tok, tok), 1)
            work = []
            if with_partner:
                near_copy(i).wait_recv()
            for h in (2 * i, 2 * i + 1):
                keys = [kv_ref[0, :, head_lanes(h)]]
                flats = [flat(kv_ref[1, :, head_lanes(h)])]
                if with_partner:
                    keys.append(near[FROM_PARTNER, 0, :, head_lanes(h)])
                    flats.append(flat(near[FROM_PARTNER, 1, :, head_lanes(h)]))
                for g in range(GROUP):
                    work.append((h * GROUP + g, [score(k, query(h, g)) for k in keys], flats))
            for n, parts, flats in work:
                parts = [jnp.where(seen, parts[0], NEG_FILL)] + parts[1:]
                top = top_of(parts)
                top_ref[n] = top
                den_ref[n], acc_ref[n] = weigh(parts, top, flats)

        return two

    def spread():
        others(lambda p: side_swap(other_row, p).wait_recv())
        when(jnp.logical_not(is_last), lambda: down(other_row).start())
        when(sends, lambda: loop(n_first, HK, behind_start))
        when(low == 1, lambda: twin(row - 1, side).start())

    def near_more():
        when(sends & starts, lambda: loop(0, HK, behind_start))
        side_swap(other_row, pair).wait_recv()
        loop(pair + 1, pairs, lambda p: up(p).start())

        def over(p):
            swap(p, p).wait_recv()
            side_swap(row, p).start()

        loop(pair + 1, pairs, over)
        loop(0, pair, lambda p: swap(p, p).wait_recv())
        when(sends & jnp.logical_not(starts), lambda: loop(0, n_first, behind_start))
        when(jnp.logical_not(is_last), lambda: down(row).start())

    def near_own(with_partner):
        two = near_first(with_partner)

        def step(i):
            if with_partner:
                when(i == 0, near_more)
            two(i)
            if with_partner:
                when(i == 0, spread)
            else:
                when(i == 0, near_more)
                when(i == 1, spread)

        loop(0, HK // 2, step)

    @pl.when(side == 0)
    def _():
        near_own(False)

    @pl.when(side == 1)
    def _():
        near_own(True)

    def mid_arrive(p):
        mid_copy(p, p).wait_recv()
        mid_pass(p, side).start()

    loop(0, pair, mid_arrive)
    loop(0, pair, lambda p: mid_pass(p, 1 - side).wait_recv())

    @pl.when(side == 1)
    def _():
        mid_pass(pair, 0).wait_recv()

    n_mid = mid_buf.shape[0]

    def mid_all():
        seen = (iota((n_mid, tok), 0) * MID + MID - 1) <= (iota((n_mid, tok), 1) + col * tok)
        work = []
        for h in range(HK):
            keys = mid_buf[:, head_lanes(h)]
            values = flat(mid_buf[:, head_lanes(h, KV)])
            for g in range(GROUP):
                work.append((h * GROUP + g, score(keys, query(h, g)), values))
        for n, s, values in work:
            s = jnp.where(seen, s, NEG_FILL)
            den, acc = weigh([s], jnp.maximum(top_of([s]), TOP_FLOOR), [values])
            rest_ref[n] = acc * inverse(den)

    mid_all()

    def hand_on(k):
        def one(i):
            r = 2 * (high - 1 - k) + lax.rem(low + i, 2)

            @pl.when(is_hub)
            def _():
                when(k == 0, lambda: down(r).wait_recv())
                when(k == 1, lambda: cross(r).wait_recv())
                when(k > 1, lambda: lift(r).wait_recv())

            @pl.when(jnp.logical_not(is_hub))
            def _():
                down(r).wait_recv()
                when(jnp.logical_not(is_last), lambda: down(r).start())
                when(feeds_beside & (k == 1), lambda: cross(r).start())
                when(feeds_next & (k > 1), lambda: lift(r).start())

            twin(r, side).start()

        loop(0, 2, one)

    def arrive(h):
        behind_copy(h).wait_recv()
        relay_copy(h).start()

    def near_last(h):
        relay_copy(h).wait_recv()
        slots = (FROM_BEHIND, RELAYED)
        keys = [near[slot, 0, :, head_lanes(h)] for slot in slots]
        flats = [flat(near[slot, 1, :, head_lanes(h)]) for slot in slots]
        work = [[score(k, query(h, g)) for k in keys] for g in range(GROUP)]
        for g, parts in enumerate(work):
            n = h * GROUP + g
            before = top_ref[n]
            top = jnp.maximum(before, top_of(parts))
            den, acc = weigh(parts, top, flats)
            fade = powers(before, top)
            den_ref[n] = den_ref[n] * fade + den
            acc_ref[n] = acc_ref[n] * fade + acc

    line = far_buf.shape[1]
    def far_chunk(j):
        def part(h, base):
            block = far_buf[pl.ds(j * SLABS, SLABS), :, head_lanes(h, base)]
            return block.reshape(SLABS * line, DH)

        seen = iota((SLABS * line, 1), 0) + j * (SLABS * line) < 2 * row * line
        work = []
        for h in range(HK):
            keys, flats = part(h, 0), flat(part(h, KV))
            work += [(h * GROUP + g, score(keys, query(h, g)), flats) for g in range(GROUP)]
        for n, s, flats in work:
            s = jnp.where(seen, s, NEG_FILL)
            before = far_top[n]
            top = jnp.maximum(before, top_of([s]))
            fade = powers(before, top)
            den, acc = weigh([s], top, [flats])
            far_top[n] = top
            far_den[n] = far_den[n] * fade + den
            far_acc[n] = far_acc[n] * fade + acc

    def far_rows(j):
        loop(2 * j, jnp.minimum(2 * j + 2, row), lambda r: twin(r, 1 - side).wait_recv())
        far_chunk(j)

    def far_back(k_low, k_high):
        loop(k_low, k_high, lambda k: far_rows(high - 1 - k))

    def finish(with_far, h):
        for g in range(GROUP):
            n = h * GROUP + g
            whole = acc_ref[n] * inverse(den_ref[n]) + rest_ref[n]
            if with_far:
                whole = whole + far_acc[n] * inverse(far_den[n])
            lanes = pl.ds(pl.multiple_of(n * DH, DH), DH)
            out_ref[:, lanes] = whole.astype(out_ref.dtype).T

    def sent_early():
        others(lambda p: swap(p, pair).wait_send())
        loop(pair + 1, pairs, lambda p: mid_copy(p, pair).wait_send())
        loop(pair, pairs, lambda p: side_swap(row, p).wait_send())
        loop(pair + 1, pairs, lambda p: up(p).wait_send())
        loop(0, pair, lambda p: mid_pass(p, side).wait_send())

        @pl.when(side == 0)
        def _():
            loop(0, 2, lambda half: near_copy(half).wait_send())
            mid_pass(pair, 0).wait_send()

    def feeds_next_done():
        @pl.when(jnp.logical_not(is_last))
        def _():
            loop(jnp.where(is_hub, 2 * high, 0), 2 * high + 2, lambda r: down(r).wait_send())

        @pl.when(feeds_beside & (high > 1))
        def _():
            loop(2 * high - 4, 2 * high - 2, lambda r: cross(r).wait_send())

        @pl.when(feeds_next)
        def _():
            loop(0, 2 * high - 4, lambda r: lift(r).wait_send())

    def near_in(h):
        when(pos >= 2, lambda: arrive(h))

    def near_end(h):
        @pl.when(pos >= 2)
        def _():
            near_last(h)

    plain = jnp.logical_not(is_hub)
    near_late = (low == 0) & (pair == 0) & (side == 0) & (high > 1)
    far_late = (low == 0) & (pair == 0) & (high > 1) & jnp.logical_not(is_last)

    def step(s):
        when((s == 0) & (high > 0) & plain, lambda: hand_on(0))
        when((s < HK) & (s != 2), lambda: near_in(s))
        when(s == 0, lambda: far_back(jnp.where(low == 1, -1, 0), jnp.where(plain & jnp.logical_not(far_late), jnp.minimum(high, 1), 0)))
        when((s == 1) & (high > 1) & plain, lambda: hand_on(1))
        when(s > 0, lambda: near_end(s - 1))

        @pl.when(s == 2)
        def _():
            loop(jnp.where(is_hub, 0, 2), jnp.where(is_hub, jnp.minimum(high, 1), high), hand_on)
            when(jnp.logical_not(near_late), lambda: near_in(2))
            far_back(jnp.where(plain & jnp.logical_not(far_late), 1, 0), jnp.where(plain, high, jnp.minimum(high, 1)))
            when(near_late, lambda: near_in(2))
            when((row > 0) & plain, lambda: loop(0, 2, functools.partial(finish, True)))

        @pl.when(s == HK - 1)
        def _():
            sent_early()
            when(is_hub & (high > 1), lambda: hand_on(1))
            when(plain & (row > 0), lambda: loop(2, HK - 1, functools.partial(finish, True)))

    loop(0, HK + 1, step)

    @pl.when(row > 0)
    def _():
        @pl.when(is_hub)
        def _():
            loop(2, high, hand_on)
            far_back(1, high)

        loop(jnp.where(is_hub, 0, HK - 1), HK, functools.partial(finish, True))

    @pl.when(row == 0)
    def _():
        loop(0, HK, functools.partial(finish, False))

    loop(0, row, lambda r: twin(r, side).wait_send())
    feeds_next_done()

    @pl.when(pos + 2 < total)
    def _():
        loop(0, HK, lambda h: behind_copy(h).wait_send())

    @pl.when(pos >= 2)
    def _():
        loop(0, HK, lambda h: relay_copy(h).wait_send())


def body(rows, cols, queries, keys, values, *weights):
    tok = queries.shape[0]
    assert BLOCK == 2 * tok and cols % 2 == 0 and rows % 2 == 0
    dma = pltpu.SemaphoreType.DMA
    bf16, f32 = jnp.bfloat16, jnp.float32
    vmem = pl.BlockSpec(memory_space=pltpu.VMEM)
    pairs = cols // 2
    return pl.pallas_call(
        functools.partial(kernel, rows, cols),
        out_shape=pltpu.VMEM(queries.shape, bf16),
        in_specs=[pl.BlockSpec(memory_space=pltpu.HBM)] * 7,
        out_specs=vmem,
        scratch_shapes=[
            pltpu.VMEM(queries.shape, bf16),
            pltpu.VMEM((2, *keys.shape), bf16),
            *[pltpu.VMEM(a.shape, a.dtype) for a in weights],
            dma((7,)),
            pltpu.VMEM((2 * HK, tok, DH), f32),
            pltpu.VMEM((cols * (tok // MID), 2 * KV), bf16),
            pltpu.VMEM((2 * rows, pairs * (tok // FAR), 2 * KV), bf16),
            pltpu.VMEM((3, 2, tok, KV), bf16),
            pltpu.VMEM((HQ, 1, tok), f32),
            pltpu.VMEM((HQ, 1, tok), f32),
            pltpu.VMEM((HQ, DH, tok), f32),
            pltpu.VMEM((HQ, DH, tok), f32),
            pltpu.VMEM((HQ, 1, tok), f32),
            pltpu.VMEM((HQ, 1, tok), f32),
            pltpu.VMEM((HQ, DH, tok), f32),
            dma((3, HK)),
            dma((3, HK)),
            *[dma((pairs,))] * 9,
            *[dma((rows,))] * 2,
            *[dma((2,))] * 2,
            *[dma((max(rows - 6, 1),))] * 2,
            *[dma((rows,))] * 2,
        ],
        compiler_params=pltpu.CompilerParams(
            collective_id=0, has_side_effects=True, vmem_limit_bytes=VMEM_LIMIT
        ),
    )(queries, keys, values, *weights)


def solution(mesh):
    spec = P(("row", "col"), None)
    return jax.shard_map(
        functools.partial(body, mesh.shape["row"], mesh.shape["col"]),
        mesh=mesh,
        in_specs=(spec, spec, spec, P(), P(), P(), P()),
        out_specs=spec,
        check_vma=False,
    )
```

```python
import functools
import math

import jax
import jax.numpy as jnp
from jax import lax
from jax.experimental import pallas as pl
from jax.experimental.pallas import tpu as pltpu
from jax.sharding import PartitionSpec as P

HQ = 16
HK = 4
DH = 128
BLOCK = 512
MID = 8
FAR = 16
GROUP = HQ // HK
KV = HK * DH
NEG_FILL = -1e30
TOP_FLOOR = -1e29
SUM_ROWS = 16
N_FIRST = 2
EXP_SCALE = DH ** (-0.5) * math.log2(math.e)
SLABS = 4
VMEM_LIMIT = 57 * 1024 * 1024
MESH = pl.DeviceIdType.MESH
FROM_BEHIND, RELAYED, FROM_PARTNER = 0, 1, 2


def score(k, q):
    return lax.dot_general(k, q, (((1,), (1,)), ((), ())), preferred_element_type=jnp.float32)


def powers(s, top):
    return jnp.exp2((s - top) * EXP_SCALE)


def top_of(parts):
    return functools.reduce(jnp.maximum, [jnp.max(s, axis=0, keepdims=True) for s in parts])


def flat(v):
    return jnp.concatenate([v.T, jnp.ones((SUM_ROWS, v.shape[0]), v.dtype)], axis=0)


def weigh(parts, top, flats):
    terms = [
        jnp.dot(v, powers(s, top).astype(jnp.bfloat16), preferred_element_type=jnp.float32)
        for s, v in zip(parts, flats)
    ]
    both = functools.reduce(jnp.add, terms)
    return both[DH:DH + 1], both[:DH]


def inverse(den):
    return 1.0 / jnp.maximum(den, 1.0)


def kernel(
    rows, cols,
    q_hbm, k_hbm, v_hbm, wmk_hbm, wmv_hbm, wfk_hbm, wfv_hbm, out_ref,
    q_ref, kv_ref, wmk_ref, wmv_ref, wfk_ref, wfv_ref, fetch_sem,
    wide, mid_buf, far_buf, near, top_ref, den_ref, acc_ref, rest_ref,
    far_top, far_den, far_acc,
    near_send, near_recv, own_sem, mid_sem, pass_send, pass_recv,
    swap_send, swap_recv, side_send, side_recv,
    down_send, down_recv, cross_send, lift_send, twin_send, twin_recv,
):
    tok = q_ref.shape[0]
    mids, fars = tok // MID, tok // FAR
    total = rows * cols
    pairs = cols // 2
    row, col = lax.axis_index("row"), lax.axis_index("col")
    pos = row * cols + col
    side = lax.rem(col, 2)
    pair = col // 2
    low = lax.rem(row, 2)
    high = row // 2
    other_row = row + 1 - 2 * low
    partner = (row, col + 1 - 2 * side)
    beside = (other_row, col)
    is_hub = (low == 1) & (pair == pairs - 1)
    feeds_beside = (low == 0) & (pair == pairs - 1)
    feeds_next = (low == 1) & (pair == pairs - 2)
    is_last = high + 1 == rows // 2

    def fetch(i, src, dst):
        return pltpu.make_async_copy(src, dst, fetch_sem.at[i])

    fetches = [
        fetch(i, src, dst)
        for i, (src, dst) in enumerate((
            (k_hbm, kv_ref.at[0]), (v_hbm, kv_ref.at[1]), (wfk_hbm, wfk_ref), (wfv_hbm, wfv_ref),
            (wmk_hbm, wmk_ref), (wmv_hbm, wmv_ref), (q_hbm, q_ref),
        ))
    ]
    for copy in fetches:
        copy.start()

    def loop(low, high, f):
        def step(i, _):
            f(i)
            return 0

        lax.fori_loop(low, high, step, 0)

    def at(linear):
        return (linear // cols, lax.rem(linear, cols))

    ahead = at(lax.rem(pos + 2, total))

    mid_buf[...] = jnp.zeros_like(mid_buf)

    far_top[...] = jnp.full_like(far_top, TOP_FLOOR)
    far_den[...] = jnp.zeros_like(far_den)

    def reset(n):
        far_acc[n] = jnp.zeros(far_acc.shape[1:], far_acc.dtype)

    loop(0, HQ, reset)

    def clear(c):
        far_buf[c] = jnp.zeros(far_buf.shape[1:], far_buf.dtype)

    loop(0, 2 * rows, clear)

    barrier = pltpu.get_barrier_semaphore()

    def greet(device):
        pl.semaphore_signal(barrier, inc=1, device_id=device, device_id_type=MESH)

    loop(1, cols, lambda i: greet((row, lax.rem(col + i, cols))))
    greet((other_row, col))

    def greet_if(condition, device):
        @pl.when(condition)
        def _():
            greet(device)

        return condition.astype(jnp.int32)

    greeted = (
        cols
        + greet_if(jnp.logical_not(is_last), (row + 2, col))
        + greet_if(high > 0, (row - 2, col))
        + greet_if(pos + 2 < total, at(pos + 2))
        + greet_if(pos >= 2, at(pos - 2))
    )

    def head_lanes(h, base=0):
        return pl.ds(pl.multiple_of(base + h * DH, DH), DH)

    def remote(src, dst, send, recv, device):
        return pltpu.make_async_remote_copy(
            src_ref=src, dst_ref=dst, send_sem=send, recv_sem=recv,
            device_id=device, device_id_type=MESH,
        )

    def same(ref, send, recv, device):
        return remote(ref, ref, send, recv, device)

    def far_block(r, p):
        return far_buf.at[2 * r + side, pl.ds(pl.multiple_of(p * fars, fars), fars), :]

    def swap(p_to, p_from):
        return same(far_block(row, p_from), swap_send.at[p_to], swap_recv.at[p_from], (row, 2 * p_to + side))

    def side_swap(r, p):
        return same(far_block(r, p), side_send.at[p], side_recv.at[p], beside)

    def up(p):
        return same(far_block(other_row, pair), pass_send.at[p], side_recv.at[pair], (row, 2 * p + side))

    def down(r):
        return same(far_buf.at[2 * r + side], down_send.at[r], down_recv.at[r], (row + 2, col))

    def cross(r):
        return same(far_buf.at[2 * r + side], cross_send.at[lax.rem(r, 2)], down_recv.at[r], beside)

    def lift(r):
        return same(far_buf.at[2 * r + side], lift_send.at[r], down_recv.at[r], (row, col + 2))

    def twin(r, s):
        return same(far_buf.at[2 * r + s], twin_send.at[r], twin_recv.at[r], partner)

    def mid_span(c):
        return mid_buf.at[pl.ds(pl.multiple_of(c * mids, mids), mids), :]

    def mid_copy(p_to, p_from):
        return same(mid_span(2 * p_from + side), mid_sem.at[p_to], mid_sem.at[p_from], (row, 2 * p_to + side))

    def mid_pass(p, s):
        return same(mid_span(2 * p + s), pass_send.at[p], pass_recv.at[p], partner)

    def near_copy(half):
        lanes = pl.ds(pl.multiple_of(half * (KV // 2), KV // 2), KV // 2)
        return remote(
            kv_ref.at[:, :, lanes], near.at[FROM_PARTNER, :, :, lanes],
            own_sem.at[half], own_sem.at[half], partner,
        )

    def behind_copy(h):
        lanes = head_lanes(h)
        return remote(
            kv_ref.at[:, :, lanes], near.at[FROM_BEHIND, :, :, lanes],
            near_send.at[FROM_BEHIND, h], near_recv.at[FROM_BEHIND, h], ahead,
        )

    def relay_copy(h):
        lanes = head_lanes(h)
        return remote(
            near.at[FROM_BEHIND, :, :, lanes], near.at[RELAYED, :, :, lanes],
            near_send.at[RELAYED, h], near_recv.at[RELAYED, h], partner,
        )

    def behind_start(h):
        behind_copy(h).start()

    mid_rows = pl.ds(pl.multiple_of(col * mids, mids), mids)
    far_rows = pl.ds(pl.multiple_of(pair * fars, fars), fars)

    def spread_out(s):
        for h in range(HK):
            wide[s * HK + h] = kv_ref[s, :, h * DH:(h + 1) * DH].astype(jnp.float32)

    def summarise(s, squeeze, weight):
        count = tok // squeeze
        grouped = jnp.concatenate(
            [
                jnp.concatenate(
                    [wide[s * HK + h, pl.ds(i, count, stride=squeeze), :] for h in range(HK)],
                    axis=0,
                ).astype(jnp.bfloat16)
                for i in range(squeeze)
            ],
            axis=1,
        )
        merged = jnp.dot(grouped, weight[...], preferred_element_type=jnp.float32)
        merged = merged.astype(jnp.bfloat16)
        for h in range(HK):
            lanes = slice(s * KV + h * DH, s * KV + (h + 1) * DH)
            piece = merged[h * count:(h + 1) * count]
            if squeeze == FAR:
                far_buf[2 * row + side, far_rows, lanes] = piece
            else:
                mid_buf[mid_rows, lanes] = piece

    def others(f):
        def one(p):
            @pl.when(p != pair)
            def _():
                f(p)

        loop(0, pairs, one)

    def when(condition, f):
        @pl.when(condition)
        def _():
            f()

    for copy in fetches[:2]:
        copy.wait()
    spread_out(0)
    spread_out(1)
    for copy in fetches[2:4]:
        copy.wait()
    summarise(0, FAR, wfk_ref)
    summarise(1, FAR, wfv_ref)
    pl.semaphore_wait(barrier, greeted)
    others(lambda p: swap(p, pair).start())
    side_swap(row, pair).start()
    when(side == 0, lambda: loop(0, 2, lambda half: near_copy(half).start()))
    for copy in fetches[4:6]:
        copy.wait()
    summarise(0, MID, wmk_ref)
    summarise(1, MID, wmv_ref)
    loop(pair + 1, pairs, lambda p: mid_copy(p, pair).start())
    when(side == 0, lambda: mid_pass(pair, 0).start())

    sends = pos + 2 < total
    n_now = (
        jnp.where(feeds_beside & (side == 0), HK, 0)
        + jnp.where((side == 0) & (low == 1) & (pair == pairs - 2), 1, 0)
        + jnp.where(is_hub & (side == 1), 1, 0)
    )
    n_first = jnp.where(is_hub, N_FIRST, HK)

    fetches[6].wait()

    def iota(shape, axis):
        return lax.broadcasted_iota(jnp.int32, shape, axis)

    def query(h, g):
        return q_ref[:, pl.ds(pl.multiple_of((h * GROUP + g) * DH, DH), DH)]

    def near_first(with_partner):
        def two(i):
            seen = iota((tok, tok), 0) <= iota((tok, tok), 1)
            work = []
            if with_partner:
                near_copy(i).wait_recv()
            for h in (2 * i, 2 * i + 1):
                keys = [kv_ref[0, :, head_lanes(h)]]
                flats = [flat(kv_ref[1, :, head_lanes(h)])]
                if with_partner:
                    keys.append(near[FROM_PARTNER, 0, :, head_lanes(h)])
                    flats.append(flat(near[FROM_PARTNER, 1, :, head_lanes(h)]))
                for g in range(GROUP):
                    work.append((h * GROUP + g, [score(k, query(h, g)) for k in keys], flats))
            for n, parts, flats in work:
                parts = [jnp.where(seen, parts[0], NEG_FILL)] + parts[1:]
                top = top_of(parts)
                top_ref[n] = top
                den_ref[n], acc_ref[n] = weigh(parts, top, flats)

        return two

    def spread():
        others(lambda p: side_swap(other_row, p).wait_recv())
        when(jnp.logical_not(is_last), lambda: down(other_row).start())
        when(sends, lambda: loop(n_first, HK, behind_start))
        when(low == 1, lambda: twin(row - 1, side).start())

    def near_more():
        when(sends, lambda: loop(0, n_now, behind_start))
        side_swap(other_row, pair).wait_recv()
        loop(pair + 1, pairs, lambda p: up(p).start())

        def over(p):
            swap(p, p).wait_recv()
            side_swap(row, p).start()

        loop(pair + 1, pairs, over)
        loop(0, pair, lambda p: swap(p, p).wait_recv())
        when(sends, lambda: loop(n_now, n_first, behind_start))
        when(jnp.logical_not(is_last), lambda: down(row).start())

    def near_own(with_partner):
        two = near_first(with_partner)

        def step(i):
            if with_partner:
                when(i == 0, near_more)
            two(i)
            if with_partner:
                when(i == 0, spread)
            else:
                when(i == 0, near_more)
                when(i == 1, spread)

        loop(0, HK // 2, step)

    @pl.when(side == 0)
    def _():
        near_own(False)

    @pl.when(side == 1)
    def _():
        near_own(True)

    def mid_arrive(p):
        mid_copy(p, p).wait_recv()
        mid_pass(p, side).start()

    loop(0, pair, mid_arrive)
    loop(0, pair, lambda p: mid_pass(p, 1 - side).wait_recv())

    @pl.when(side == 1)
    def _():
        mid_pass(pair, 0).wait_recv()

    n_mid = mid_buf.shape[0]

    def mid_all():
        seen = (iota((n_mid, tok), 0) * MID + MID - 1) <= (iota((n_mid, tok), 1) + col * tok)
        work = []
        for h in range(HK):
            keys = mid_buf[:, head_lanes(h)]
            values = flat(mid_buf[:, head_lanes(h, KV)])
            for g in range(GROUP):
                work.append((h * GROUP + g, score(keys, query(h, g)), values))
        for n, s, values in work:
            s = jnp.where(seen, s, NEG_FILL)
            den, acc = weigh([s], jnp.maximum(top_of([s]), TOP_FLOOR), [values])
            rest_ref[n] = acc * inverse(den)

    mid_all()

    def hand_on(k):
        def one(i):
            r = 2 * (high - 1 - k) + lax.rem(low + i, 2)

            @pl.when(is_hub)
            def _():
                when(k == 0, lambda: down(r).wait_recv())
                when(k == 1, lambda: cross(r).wait_recv())
                when(k > 1, lambda: lift(r).wait_recv())

            @pl.when(jnp.logical_not(is_hub))
            def _():
                down(r).wait_recv()
                when(jnp.logical_not(is_last), lambda: down(r).start())
                when(feeds_beside & (k == 1), lambda: cross(r).start())
                when(feeds_next & (k > 1), lambda: lift(r).start())

            twin(r, side).start()

        loop(0, 2, one)

    def arrive(h):
        behind_copy(h).wait_recv()
        relay_copy(h).start()

    def near_last(h):
        relay_copy(h).wait_recv()
        slots = (FROM_BEHIND, RELAYED)
        keys = [near[slot, 0, :, head_lanes(h)] for slot in slots]
        flats = [flat(near[slot, 1, :, head_lanes(h)]) for slot in slots]
        work = [[score(k, query(h, g)) for k in keys] for g in range(GROUP)]
        for g, parts in enumerate(work):
            n = h * GROUP + g
            before = top_ref[n]
            top = jnp.maximum(before, top_of(parts))
            den, acc = weigh(parts, top, flats)
            fade = powers(before, top)
            den_ref[n] = den_ref[n] * fade + den
            acc_ref[n] = acc_ref[n] * fade + acc

    line = far_buf.shape[1]
    def put(n, whole):
        lanes = pl.ds(pl.multiple_of(n * DH, DH), DH)
        out_ref[:, lanes] = whole.astype(out_ref.dtype).T

    def far_chunk(j, last=False):
        def part(h, base):
            block = far_buf[pl.ds(j * SLABS, SLABS), :, head_lanes(h, base)]
            return block.reshape(SLABS * line, DH)

        seen = iota((SLABS * line, 1), 0) + j * (SLABS * line) < 2 * row * line
        work = []
        for h in range(HK):
            keys, flats = part(h, 0), flat(part(h, KV))
            work += [(h * GROUP + g, score(keys, query(h, g)), flats) for g in range(GROUP)]
        for n, s, flats in work:
            s = jnp.where(seen, s, NEG_FILL)
            before = far_top[n]
            top = jnp.maximum(before, top_of([s]))
            fade = powers(before, top)
            den, acc = weigh([s], top, [flats])
            den, acc = far_den[n] * fade + den, far_acc[n] * fade + acc
            if last:
                put(n, acc_ref[n] * inverse(den_ref[n]) + rest_ref[n] + acc * inverse(den))
            else:
                far_top[n], far_den[n], far_acc[n] = top, den, acc

    def far_rows(j, last=False):
        loop(2 * j, jnp.minimum(2 * j + 2, row), lambda r: twin(r, 1 - side).wait_recv())
        far_chunk(j, last)

    def far_back(k_low, k_high):
        loop(k_low, k_high, lambda k: far_rows(high - 1 - k))

    def finish(with_far, h):
        for g in range(GROUP):
            n = h * GROUP + g
            whole = acc_ref[n] * inverse(den_ref[n]) + rest_ref[n]
            if with_far:
                whole = whole + far_acc[n] * inverse(far_den[n])
            put(n, whole)

    def sent_early():
        others(lambda p: swap(p, pair).wait_send())
        loop(pair + 1, pairs, lambda p: mid_copy(p, pair).wait_send())
        loop(pair, pairs, lambda p: side_swap(row, p).wait_send())
        loop(pair + 1, pairs, lambda p: up(p).wait_send())
        loop(0, pair, lambda p: mid_pass(p, side).wait_send())

        @pl.when(side == 0)
        def _():
            loop(0, 2, lambda half: near_copy(half).wait_send())
            mid_pass(pair, 0).wait_send()

    def feeds_next_done():
        @pl.when(jnp.logical_not(is_last))
        def _():
            loop(jnp.where(is_hub, 2 * high, 0), 2 * high + 2, lambda r: down(r).wait_send())

        @pl.when(feeds_beside & (high > 1))
        def _():
            loop(2 * high - 4, 2 * high - 2, lambda r: cross(r).wait_send())

        @pl.when(feeds_next)
        def _():
            loop(0, 2 * high - 4, lambda r: lift(r).wait_send())

    def near_in(h):
        when(pos >= 2, lambda: arrive(h))

    def near_end(h):
        @pl.when(pos >= 2)
        def _():
            near_last(h)

    plain = jnp.logical_not(is_hub)
    near_late = (low == 0) & (pair == 0) & (side == 0) & (high > 1)
    far_late = (low == 0) & (pair == 0) & (high > 1) & jnp.logical_not(is_last)

    def step(s):
        when((s == 0) & (high > 0) & plain, lambda: hand_on(0))
        when((s < HK) & (s != 2), lambda: near_in(s))
        when(s == 0, lambda: far_back(jnp.where(low == 1, -1, 0), jnp.where(plain & jnp.logical_not(far_late), jnp.minimum(high, 1), 0)))
        when((s == 1) & (high > 1) & plain, lambda: hand_on(1))
        when(s > 0, lambda: near_end(s - 1))

        @pl.when(s == 2)
        def _():
            loop(jnp.where(is_hub, 0, 2), jnp.where(is_hub, jnp.minimum(high, 1), high), hand_on)
            first = jnp.where(plain & jnp.logical_not(far_late), 1, 0)
            split = jnp.where(near_late, first + 1, first)
            far_back(first, split)
            near_in(2)
            far_back(split, jnp.where(plain, high, jnp.minimum(high, 1)))
            when((row > 0) & plain, lambda: loop(0, 2, functools.partial(finish, True)))

        @pl.when(s == HK - 1)
        def _():
            sent_early()
            when(is_hub & (high > 1), lambda: hand_on(1))
            when(plain & (row > 0), lambda: loop(2, HK - 1, functools.partial(finish, True)))

    loop(0, HK + 1, step)

    @pl.when(row > 0)
    def _():
        ends_far = is_hub & (high > 1)

        @pl.when(ends_far)
        def _():
            loop(2, high, hand_on)
            far_back(1, high - 1)
            far_rows(0, True)

        @pl.when(jnp.logical_not(ends_far))
        def _():
            loop(jnp.where(is_hub, 0, HK - 1), HK, functools.partial(finish, True))

    @pl.when(row == 0)
    def _():
        loop(0, HK, functools.partial(finish, False))

    loop(0, row, lambda r: twin(r, side).wait_send())
    feeds_next_done()

    @pl.when(pos + 2 < total)
    def _():
        loop(0, HK, lambda h: behind_copy(h).wait_send())

    @pl.when(pos >= 2)
    def _():
        loop(0, HK, lambda h: relay_copy(h).wait_send())


def body(rows, cols, queries, keys, values, *weights):
    tok = queries.shape[0]
    assert BLOCK == 2 * tok and cols % 2 == 0 and rows % 2 == 0
    dma = pltpu.SemaphoreType.DMA
    bf16, f32 = jnp.bfloat16, jnp.float32
    vmem = pl.BlockSpec(memory_space=pltpu.VMEM)
    pairs = cols // 2
    return pl.pallas_call(
        functools.partial(kernel, rows, cols),
        out_shape=pltpu.VMEM(queries.shape, bf16),
        in_specs=[pl.BlockSpec(memory_space=pltpu.HBM)] * 7,
        out_specs=vmem,
        scratch_shapes=[
            pltpu.VMEM(queries.shape, bf16),
            pltpu.VMEM((2, *keys.shape), bf16),
            *[pltpu.VMEM(a.shape, a.dtype) for a in weights],
            dma((7,)),
            pltpu.VMEM((2 * HK, tok, DH), f32),
            pltpu.VMEM((cols * (tok // MID), 2 * KV), bf16),
            pltpu.VMEM((2 * rows, pairs * (tok // FAR), 2 * KV), bf16),
            pltpu.VMEM((3, 2, tok, KV), bf16),
            pltpu.VMEM((HQ, 1, tok), f32),
            pltpu.VMEM((HQ, 1, tok), f32),
            pltpu.VMEM((HQ, DH, tok), f32),
            pltpu.VMEM((HQ, DH, tok), f32),
            pltpu.VMEM((HQ, 1, tok), f32),
            pltpu.VMEM((HQ, 1, tok), f32),
            pltpu.VMEM((HQ, DH, tok), f32),
            dma((2, HK)),
            dma((2, HK)),
            dma((2,)),
            *[dma((pairs,))] * 7,
            *[dma((rows,))] * 2,
            dma((2,)),
            dma((max(rows - 6, 1),)),
            *[dma((rows,))] * 2,
        ],
        compiler_params=pltpu.CompilerParams(
            collective_id=0, has_side_effects=True, vmem_limit_bytes=VMEM_LIMIT
        ),
    )(queries, keys, values, *weights)


def solution(mesh):
    spec = P(("row", "col"), None)
    return jax.shard_map(
        functools.partial(body, mesh.shape["row"], mesh.shape["col"]),
        mesh=mesh,
        in_specs=(spec, spec, spec, P(), P(), P(), P()),
        out_specs=spec,
        check_vma=False,
    )
```

```python
import functools
import math

import jax
import jax.numpy as jnp
from jax import lax
from jax.experimental import pallas as pl
from jax.experimental.pallas import tpu as pltpu
from jax.sharding import PartitionSpec as P

HQ = 16
HK = 4
DH = 128
BLOCK = 512
MID = 8
FAR = 16
GROUP = HQ // HK
KV = HK * DH
NEG_FILL = -1e30
TOP_FLOOR = -1e29
SUM_ROWS = 16
N_FIRST = 2
EXP_SCALE = DH ** (-0.5) * math.log2(math.e)
SLABS = 4
VMEM_LIMIT = 57 * 1024 * 1024
MESH = pl.DeviceIdType.MESH
FROM_BEHIND, RELAYED, FROM_PARTNER = 0, 1, 2


def score(k, q):
    return lax.dot_general(k, q, (((1,), (1,)), ((), ())), preferred_element_type=jnp.float32)


def powers(s, top):
    return jnp.exp2((s - top) * EXP_SCALE)


def top_of(parts):
    return functools.reduce(jnp.maximum, [jnp.max(s, axis=0, keepdims=True) for s in parts])


def flat(v):
    return jnp.concatenate([v.T, jnp.ones((SUM_ROWS, v.shape[0]), v.dtype)], axis=0)


def weigh(parts, top, flats):
    terms = [
        jnp.dot(v, powers(s, top).astype(jnp.bfloat16), preferred_element_type=jnp.float32)
        for s, v in zip(parts, flats)
    ]
    both = functools.reduce(jnp.add, terms)
    return both[DH:DH + 1], both[:DH]


def inverse(den):
    return 1.0 / jnp.maximum(den, 1.0)


def kernel(
    rows, cols,
    q_hbm, k_hbm, v_hbm, wmk_hbm, wmv_hbm, wfk_hbm, wfv_hbm, out_ref,
    q_ref, kv_ref, wmk_ref, wmv_ref, wfk_ref, wfv_ref, fetch_sem,
    wide, mid_buf, far_buf, near, top_ref, den_ref, acc_ref, rest_ref,
    far_top, far_den, far_acc,
    near_send, near_recv, own_sem, mid_sem, pass_send, pass_recv,
    swap_send, swap_recv, side_send, side_recv,
    down_send, down_recv, cross_send, lift_send, twin_send, twin_recv,
):
    tok = q_ref.shape[0]
    mids, fars = tok // MID, tok // FAR
    total = rows * cols
    pairs = cols // 2
    row, col = lax.axis_index("row"), lax.axis_index("col")
    pos = row * cols + col
    side = lax.rem(col, 2)
    pair = col // 2
    low = lax.rem(row, 2)
    high = row // 2
    other_row = row + 1 - 2 * low
    partner = (row, col + 1 - 2 * side)
    beside = (other_row, col)
    is_hub = (low == 1) & (pair == pairs - 1)
    feeds_beside = (low == 0) & (pair == pairs - 1)
    feeds_next = (low == 1) & (pair == pairs - 2)
    is_last = high + 1 == rows // 2

    def fetch(i, src, dst):
        return pltpu.make_async_copy(src, dst, fetch_sem.at[i])

    fetches = [
        fetch(i, src, dst)
        for i, (src, dst) in enumerate((
            (k_hbm, kv_ref.at[0]), (v_hbm, kv_ref.at[1]), (wfk_hbm, wfk_ref), (wfv_hbm, wfv_ref),
            (wmk_hbm, wmk_ref), (wmv_hbm, wmv_ref), (q_hbm, q_ref),
        ))
    ]
    for copy in fetches:
        copy.start()

    def loop(low, high, f):
        def step(i, _):
            f(i)
            return 0

        lax.fori_loop(low, high, step, 0)

    def at(linear):
        return (linear // cols, lax.rem(linear, cols))

    ahead = at(lax.rem(pos + 2, total))

    mid_buf[...] = jnp.zeros_like(mid_buf)

    far_top[...] = jnp.full_like(far_top, TOP_FLOOR)
    far_den[...] = jnp.zeros_like(far_den)

    def reset(n):
        far_acc[n] = jnp.zeros(far_acc.shape[1:], far_acc.dtype)

    loop(0, HQ, reset)

    def clear(c):
        far_buf[c] = jnp.zeros(far_buf.shape[1:], far_buf.dtype)

    loop(0, 2 * rows, clear)

    barrier = pltpu.get_barrier_semaphore()

    def greet(device):
        pl.semaphore_signal(barrier, inc=1, device_id=device, device_id_type=MESH)

    loop(1, cols, lambda i: greet((row, lax.rem(col + i, cols))))
    greet((other_row, col))

    def greet_if(condition, device):
        @pl.when(condition)
        def _():
            greet(device)

        return condition.astype(jnp.int32)

    greeted = (
        cols
        + greet_if(jnp.logical_not(is_last), (row + 2, col))
        + greet_if(high > 0, (row - 2, col))
        + greet_if(pos + 2 < total, at(pos + 2))
        + greet_if(pos >= 2, at(pos - 2))
    )

    def head_lanes(h, base=0):
        return pl.ds(pl.multiple_of(base + h * DH, DH), DH)

    def remote(src, dst, send, recv, device):
        return pltpu.make_async_remote_copy(
            src_ref=src, dst_ref=dst, send_sem=send, recv_sem=recv,
            device_id=device, device_id_type=MESH,
        )

    def same(ref, send, recv, device):
        return remote(ref, ref, send, recv, device)

    def far_block(r, p):
        return far_buf.at[2 * r + side, pl.ds(pl.multiple_of(p * fars, fars), fars), :]

    def swap(p_to, p_from):
        return same(far_block(row, p_from), swap_send.at[p_to], swap_recv.at[p_from], (row, 2 * p_to + side))

    def side_swap(r, p):
        return same(far_block(r, p), side_send.at[p], side_recv.at[p], beside)

    def up(p):
        return same(far_block(other_row, pair), pass_send.at[p], side_recv.at[pair], (row, 2 * p + side))

    def down(r):
        return same(far_buf.at[2 * r + side], down_send.at[r], down_recv.at[r], (row + 2, col))

    def cross(r):
        return same(far_buf.at[2 * r + side], cross_send.at[lax.rem(r, 2)], down_recv.at[r], beside)

    def lift(r):
        return same(far_buf.at[2 * r + side], lift_send.at[r], down_recv.at[r], (row, col + 2))

    def twin(r, s):
        return same(far_buf.at[2 * r + s], twin_send.at[r], twin_recv.at[r], partner)

    def mid_span(c):
        return mid_buf.at[pl.ds(pl.multiple_of(c * mids, mids), mids), :]

    def mid_copy(p_to, p_from):
        return same(mid_span(2 * p_from + side), mid_sem.at[p_to], mid_sem.at[p_from], (row, 2 * p_to + side))

    def mid_pass(p, s):
        return same(mid_span(2 * p + s), pass_send.at[p], pass_recv.at[p], partner)

    def near_copy(half):
        lanes = pl.ds(pl.multiple_of(half * (KV // 2), KV // 2), KV // 2)
        return remote(
            kv_ref.at[:, :, lanes], near.at[FROM_PARTNER, :, :, lanes],
            own_sem.at[half], own_sem.at[half], partner,
        )

    def behind_copy(h):
        lanes = head_lanes(h)
        return remote(
            kv_ref.at[:, :, lanes], near.at[FROM_BEHIND, :, :, lanes],
            near_send.at[FROM_BEHIND, h], near_recv.at[FROM_BEHIND, h], ahead,
        )

    def relay_copy(h):
        lanes = head_lanes(h)
        return remote(
            near.at[FROM_BEHIND, :, :, lanes], near.at[RELAYED, :, :, lanes],
            near_send.at[RELAYED, h], near_recv.at[RELAYED, h], partner,
        )

    def behind_start(h):
        behind_copy(h).start()

    mid_rows = pl.ds(pl.multiple_of(col * mids, mids), mids)
    far_rows = pl.ds(pl.multiple_of(pair * fars, fars), fars)

    def spread_out(s):
        for h in range(HK):
            wide[s * HK + h] = kv_ref[s, :, h * DH:(h + 1) * DH].astype(jnp.float32)

    def summarise(s, squeeze, weight):
        count = tok // squeeze
        grouped = jnp.concatenate(
            [
                jnp.concatenate(
                    [wide[s * HK + h, pl.ds(i, count, stride=squeeze), :] for h in range(HK)],
                    axis=0,
                ).astype(jnp.bfloat16)
                for i in range(squeeze)
            ],
            axis=1,
        )
        merged = jnp.dot(grouped, weight[...], preferred_element_type=jnp.float32)
        merged = merged.astype(jnp.bfloat16)
        for h in range(HK):
            lanes = slice(s * KV + h * DH, s * KV + (h + 1) * DH)
            piece = merged[h * count:(h + 1) * count]
            if squeeze == FAR:
                far_buf[2 * row + side, far_rows, lanes] = piece
            else:
                mid_buf[mid_rows, lanes] = piece

    def others(f):
        def one(p):
            @pl.when(p != pair)
            def _():
                f(p)

        loop(0, pairs, one)

    def when(condition, f):
        @pl.when(condition)
        def _():
            f()

    for copy in fetches[:2]:
        copy.wait()
    spread_out(0)
    spread_out(1)
    for copy in fetches[2:4]:
        copy.wait()
    summarise(0, FAR, wfk_ref)
    summarise(1, FAR, wfv_ref)
    pl.semaphore_wait(barrier, greeted)
    others(lambda p: swap(p, pair).start())
    side_swap(row, pair).start()
    when(side == 0, lambda: loop(0, 2, lambda half: near_copy(half).start()))
    for copy in fetches[4:6]:
        copy.wait()
    summarise(0, MID, wmk_ref)
    summarise(1, MID, wmv_ref)
    loop(pair + 1, pairs, lambda p: mid_copy(p, pair).start())
    when(side == 0, lambda: mid_pass(pair, 0).start())

    sends = pos + 2 < total
    starts = feeds_beside & (side == 0)
    n_first = jnp.where(is_hub, N_FIRST, HK)

    fetches[6].wait()

    def iota(shape, axis):
        return lax.broadcasted_iota(jnp.int32, shape, axis)

    def query(h, g):
        return q_ref[:, pl.ds(pl.multiple_of((h * GROUP + g) * DH, DH), DH)]

    def near_first(with_partner):
        def two(i):
            seen = iota((tok, tok), 0) <= iota((tok, tok), 1)
            work = []
            if with_partner:
                near_copy(i).wait_recv()
            for h in (2 * i, 2 * i + 1):
                keys = [kv_ref[0, :, head_lanes(h)]]
                flats = [flat(kv_ref[1, :, head_lanes(h)])]
                if with_partner:
                    keys.append(near[FROM_PARTNER, 0, :, head_lanes(h)])
                    flats.append(flat(near[FROM_PARTNER, 1, :, head_lanes(h)]))
                for g in range(GROUP):
                    work.append((h * GROUP + g, [score(k, query(h, g)) for k in keys], flats))
            for n, parts, flats in work:
                parts = [jnp.where(seen, parts[0], NEG_FILL)] + parts[1:]
                top = top_of(parts)
                top_ref[n] = top
                den_ref[n], acc_ref[n] = weigh(parts, top, flats)

        return two

    def spread():
        others(lambda p: side_swap(other_row, p).wait_recv())
        when(jnp.logical_not(is_last), lambda: down(other_row).start())
        when(sends, lambda: loop(n_first, HK, behind_start))
        when(low == 1, lambda: twin(row - 1, side).start())

    def near_more():
        when(sends & starts, lambda: loop(0, HK, behind_start))
        side_swap(other_row, pair).wait_recv()
        loop(pair + 1, pairs, lambda p: up(p).start())

        def over(p):
            swap(p, p).wait_recv()
            side_swap(row, p).start()

        loop(pair + 1, pairs, over)
        loop(0, pair, lambda p: swap(p, p).wait_recv())
        when(sends & jnp.logical_not(starts), lambda: loop(0, n_first, behind_start))
        when(jnp.logical_not(is_last), lambda: down(row).start())

    def near_own(with_partner):
        two = near_first(with_partner)

        def step(i):
            if with_partner:
                when(i == 0, near_more)
            two(i)
            if with_partner:
                when(i == 0, spread)
            else:
                when(i == 0, near_more)
                when(i == 1, spread)

        loop(0, HK // 2, step)

    @pl.when(side == 0)
    def _():
        near_own(False)

    @pl.when(side == 1)
    def _():
        near_own(True)

    def mid_arrive(p):
        mid_copy(p, p).wait_recv()
        mid_pass(p, side).start()

    loop(0, pair, mid_arrive)
    loop(0, pair, lambda p: mid_pass(p, 1 - side).wait_recv())

    @pl.when(side == 1)
    def _():
        mid_pass(pair, 0).wait_recv()

    n_mid = mid_buf.shape[0]

    def mid_all():
        seen = (iota((n_mid, tok), 0) * MID + MID - 1) <= (iota((n_mid, tok), 1) + col * tok)
        work = []
        for h in range(HK):
            keys = mid_buf[:, head_lanes(h)]
            values = flat(mid_buf[:, head_lanes(h, KV)])
            for g in range(GROUP):
                work.append((h * GROUP + g, score(keys, query(h, g)), values))
        for n, s, values in work:
            s = jnp.where(seen, s, NEG_FILL)
            den, acc = weigh([s], jnp.maximum(top_of([s]), TOP_FLOOR), [values])
            rest_ref[n] = acc * inverse(den)

    mid_all()

    def hand_on(k):
        def one(i):
            r = 2 * (high - 1 - k) + lax.rem(low + i, 2)

            @pl.when(is_hub)
            def _():
                when(k == 0, lambda: down(r).wait_recv())
                when(k == 1, lambda: cross(r).wait_recv())
                when(k > 1, lambda: lift(r).wait_recv())

            @pl.when(jnp.logical_not(is_hub))
            def _():
                down(r).wait_recv()
                when(jnp.logical_not(is_last), lambda: down(r).start())
                when(feeds_beside & (k == 1), lambda: cross(r).start())
                when(feeds_next & (k > 1), lambda: lift(r).start())

            twin(r, side).start()

        loop(0, 2, one)

    def arrive(h):
        behind_copy(h).wait_recv()
        relay_copy(h).start()

    def near_last(h):
        relay_copy(h).wait_recv()
        slots = (FROM_BEHIND, RELAYED)
        keys = [near[slot, 0, :, head_lanes(h)] for slot in slots]
        flats = [flat(near[slot, 1, :, head_lanes(h)]) for slot in slots]
        work = [[score(k, query(h, g)) for k in keys] for g in range(GROUP)]
        for g, parts in enumerate(work):
            n = h * GROUP + g
            before = top_ref[n]
            top = jnp.maximum(before, top_of(parts))
            den, acc = weigh(parts, top, flats)
            fade = powers(before, top)
            den_ref[n] = den_ref[n] * fade + den
            acc_ref[n] = acc_ref[n] * fade + acc

    line = far_buf.shape[1]
    def put(n, whole):
        lanes = pl.ds(pl.multiple_of(n * DH, DH), DH)
        out_ref[:, lanes] = whole.astype(out_ref.dtype).T

    def far_chunk(j, last=False):
        def part(h, base):
            block = far_buf[pl.ds(j * SLABS, SLABS), :, head_lanes(h, base)]
            return block.reshape(SLABS * line, DH)

        seen = iota((SLABS * line, 1), 0) + j * (SLABS * line) < 2 * row * line
        work = []
        for h in range(HK):
            keys, flats = part(h, 0), flat(part(h, KV))
            work += [(h * GROUP + g, score(keys, query(h, g)), flats) for g in range(GROUP)]
        for n, s, flats in work:
            s = jnp.where(seen, s, NEG_FILL)
            before = far_top[n]
            top = jnp.maximum(before, top_of([s]))
            fade = powers(before, top)
            den, acc = weigh([s], top, [flats])
            den, acc = far_den[n] * fade + den, far_acc[n] * fade + acc
            if last:
                put(n, acc_ref[n] * inverse(den_ref[n]) + rest_ref[n] + acc * inverse(den))
            else:
                far_top[n], far_den[n], far_acc[n] = top, den, acc

    def far_rows(j, last=False):
        loop(2 * j, jnp.minimum(2 * j + 2, row), lambda r: twin(r, 1 - side).wait_recv())
        far_chunk(j, last)

    def far_back(k_low, k_high):
        loop(k_low, k_high, lambda k: far_rows(high - 1 - k))

    def finish(with_far, h):
        for g in range(GROUP):
            n = h * GROUP + g
            whole = acc_ref[n] * inverse(den_ref[n]) + rest_ref[n]
            if with_far:
                whole = whole + far_acc[n] * inverse(far_den[n])
            put(n, whole)

    def sent_early():
        others(lambda p: swap(p, pair).wait_send())
        loop(pair + 1, pairs, lambda p: mid_copy(p, pair).wait_send())
        loop(pair, pairs, lambda p: side_swap(row, p).wait_send())
        loop(pair + 1, pairs, lambda p: up(p).wait_send())
        loop(0, pair, lambda p: mid_pass(p, side).wait_send())

        @pl.when(side == 0)
        def _():
            loop(0, 2, lambda half: near_copy(half).wait_send())
            mid_pass(pair, 0).wait_send()

    def feeds_next_done():
        @pl.when(jnp.logical_not(is_last))
        def _():
            loop(jnp.where(is_hub, 2 * high, 0), 2 * high + 2, lambda r: down(r).wait_send())

        @pl.when(feeds_beside & (high > 1))
        def _():
            loop(2 * high - 4, 2 * high - 2, lambda r: cross(r).wait_send())

        @pl.when(feeds_next)
        def _():
            loop(0, 2 * high - 4, lambda r: lift(r).wait_send())

    def near_in(h):
        when(pos >= 2, lambda: arrive(h))

    def near_end(h):
        @pl.when(pos >= 2)
        def _():
            near_last(h)

    plain = jnp.logical_not(is_hub)
    near_late = (low == 0) & (pair == 0) & (side == 0) & (high > 1)
    far_late = (low == 0) & (pair == 0) & (high > 1) & jnp.logical_not(is_last)

    def step(s):
        when((s == 0) & (high > 0) & plain, lambda: hand_on(0))
        when((s < HK) & (s != 2), lambda: near_in(s))
        when(s == 0, lambda: far_back(jnp.where(low == 1, -1, 0), jnp.where(plain & jnp.logical_not(far_late), jnp.minimum(high, 1), 0)))
        when((s == 1) & (high > 1) & plain, lambda: hand_on(1))
        when(s > 0, lambda: near_end(s - 1))

        @pl.when(s == 2)
        def _():
            loop(jnp.where(is_hub, 0, 2), jnp.where(is_hub, jnp.minimum(high, 1), high), hand_on)
            first = jnp.where(plain & jnp.logical_not(far_late), 1, 0)
            split = jnp.where(near_late, first + 1, first)
            far_back(first, split)
            near_in(2)
            far_back(split, jnp.where(plain, high, jnp.minimum(high, 1)))
            when((row > 0) & plain, lambda: loop(0, 2, functools.partial(finish, True)))

        @pl.when(s == HK - 1)
        def _():
            sent_early()
            when(is_hub & (high > 1), lambda: hand_on(1))
            when(plain & (row > 0), lambda: loop(2, HK - 1, functools.partial(finish, True)))

    loop(0, HK + 1, step)

    @pl.when(row > 0)
    def _():
        ends_far = is_hub & (high > 1)

        @pl.when(ends_far)
        def _():
            loop(2, high, hand_on)
            far_back(1, high - 1)
            far_rows(0, True)

        @pl.when(jnp.logical_not(ends_far))
        def _():
            loop(jnp.where(is_hub, 0, HK - 1), HK, functools.partial(finish, True))

    @pl.when(row == 0)
    def _():
        loop(0, HK, functools.partial(finish, False))

    loop(0, row, lambda r: twin(r, side).wait_send())
    feeds_next_done()

    @pl.when(pos + 2 < total)
    def _():
        loop(0, HK, lambda h: behind_copy(h).wait_send())

    @pl.when(pos >= 2)
    def _():
        loop(0, HK, lambda h: relay_copy(h).wait_send())


def body(rows, cols, queries, keys, values, *weights):
    tok = queries.shape[0]
    assert BLOCK == 2 * tok and cols % 2 == 0 and rows % 2 == 0
    dma = pltpu.SemaphoreType.DMA
    bf16, f32 = jnp.bfloat16, jnp.float32
    vmem = pl.BlockSpec(memory_space=pltpu.VMEM)
    pairs = cols // 2
    return pl.pallas_call(
        functools.partial(kernel, rows, cols),
        out_shape=pltpu.VMEM(queries.shape, bf16),
        in_specs=[pl.BlockSpec(memory_space=pltpu.HBM)] * 7,
        out_specs=vmem,
        scratch_shapes=[
            pltpu.VMEM(queries.shape, bf16),
            pltpu.VMEM((2, *keys.shape), bf16),
            *[pltpu.VMEM(a.shape, a.dtype) for a in weights],
            dma((7,)),
            pltpu.VMEM((2 * HK, tok, DH), f32),
            pltpu.VMEM((cols * (tok // MID), 2 * KV), bf16),
            pltpu.VMEM((2 * rows, pairs * (tok // FAR), 2 * KV), bf16),
            pltpu.VMEM((3, 2, tok, KV), bf16),
            pltpu.VMEM((HQ, 1, tok), f32),
            pltpu.VMEM((HQ, 1, tok), f32),
            pltpu.VMEM((HQ, DH, tok), f32),
            pltpu.VMEM((HQ, DH, tok), f32),
            pltpu.VMEM((HQ, 1, tok), f32),
            pltpu.VMEM((HQ, 1, tok), f32),
            pltpu.VMEM((HQ, DH, tok), f32),
            dma((2, HK)),
            dma((2, HK)),
            dma((2,)),
            *[dma((pairs,))] * 7,
            *[dma((rows,))] * 2,
            dma((2,)),
            dma((max(rows - 6, 1),)),
            *[dma((rows,))] * 2,
        ],
        compiler_params=pltpu.CompilerParams(
            collective_id=0, has_side_effects=True, vmem_limit_bytes=VMEM_LIMIT
        ),
    )(queries, keys, values, *weights)


def solution(mesh):
    spec = P(("row", "col"), None)
    return jax.shard_map(
        functools.partial(body, mesh.shape["row"], mesh.shape["col"]),
        mesh=mesh,
        in_specs=(spec, spec, spec, P(), P(), P(), P()),
        out_specs=spec,
        check_vma=False,
    )
```

```python
import functools
import math

import jax
import jax.numpy as jnp
from jax import lax
from jax.experimental import pallas as pl
from jax.experimental.pallas import tpu as pltpu
from jax.sharding import PartitionSpec as P

HQ = 16
HK = 4
DH = 128
BLOCK = 512
MID = 8
FAR = 16
GROUP = HQ // HK
KV = HK * DH
NEG_FILL = -1e30
TOP_FLOOR = -1e29
SUM_ROWS = 16
N_FIRST = 2
EXP_SCALE = DH ** (-0.5) * math.log2(math.e)
SLABS = 4
VMEM_LIMIT = 57 * 1024 * 1024
MESH = pl.DeviceIdType.MESH
FROM_BEHIND, RELAYED, FROM_PARTNER = 0, 1, 2


def score(k, q):
    return lax.dot_general(k, q, (((1,), (1,)), ((), ())), preferred_element_type=jnp.float32)


def powers(s, top):
    return jnp.exp2((s - top) * EXP_SCALE)


def top_of(parts):
    return functools.reduce(jnp.maximum, [jnp.max(s, axis=0, keepdims=True) for s in parts])


def flat(v):
    return jnp.concatenate([v.T, jnp.ones((SUM_ROWS, v.shape[0]), v.dtype)], axis=0)


def weigh(parts, top, flats):
    terms = [
        jnp.dot(v, powers(s, top).astype(jnp.bfloat16), preferred_element_type=jnp.float32)
        for s, v in zip(parts, flats)
    ]
    both = functools.reduce(jnp.add, terms)
    return both[DH:DH + 1], both[:DH]


def inverse(den):
    return 1.0 / jnp.maximum(den, 1.0)


def kernel(
    rows, cols,
    q_hbm, k_hbm, v_hbm, wmk_hbm, wmv_hbm, wfk_hbm, wfv_hbm, out_ref,
    q_ref, kv_ref, wmk_ref, wmv_ref, wfk_ref, wfv_ref, fetch_sem,
    wide, mid_buf, far_buf, near, top_ref, den_ref, acc_ref, rest_ref,
    far_top, far_den, far_acc,
    near_send, near_recv, own_sem, mid_sem, pass_send, pass_recv,
    swap_send, swap_recv, side_send, side_recv,
    down_send, down_recv, cross_send, lift_send, twin_send, twin_recv,
):
    tok = q_ref.shape[0]
    mids, fars = tok // MID, tok // FAR
    total = rows * cols
    pairs = cols // 2
    row, col = lax.axis_index("row"), lax.axis_index("col")
    pos = row * cols + col
    side = lax.rem(col, 2)
    pair = col // 2
    low = lax.rem(row, 2)
    high = row // 2
    other_row = row + 1 - 2 * low
    partner = (row, col + 1 - 2 * side)
    beside = (other_row, col)
    is_hub = (low == 1) & (pair == pairs - 1)
    feeds_beside = (low == 0) & (pair == pairs - 1)
    feeds_next = (low == 1) & (pair == pairs - 2)
    is_last = high + 1 == rows // 2

    def fetch(i, src, dst):
        return pltpu.make_async_copy(src, dst, fetch_sem.at[i])

    fetches = [
        fetch(i, src, dst)
        for i, (src, dst) in enumerate((
            (k_hbm, kv_ref.at[0]), (v_hbm, kv_ref.at[1]), (wfk_hbm, wfk_ref), (wfv_hbm, wfv_ref),
            (wmk_hbm, wmk_ref), (wmv_hbm, wmv_ref), (q_hbm, q_ref),
        ))
    ]
    for copy in fetches:
        copy.start()

    def loop(low, high, f):
        def step(i, _):
            f(i)
            return 0

        lax.fori_loop(low, high, step, 0)

    def at(linear):
        return (linear // cols, lax.rem(linear, cols))

    ahead = at(lax.rem(pos + 2, total))

    mid_buf[...] = jnp.zeros_like(mid_buf)

    far_top[...] = jnp.full_like(far_top, TOP_FLOOR)
    far_den[...] = jnp.zeros_like(far_den)

    def reset(n):
        far_acc[n] = jnp.zeros(far_acc.shape[1:], far_acc.dtype)

    loop(0, HQ, reset)

    def clear(c):
        far_buf[c] = jnp.zeros(far_buf.shape[1:], far_buf.dtype)

    loop(0, 2 * rows, clear)

    barrier = pltpu.get_barrier_semaphore()

    def greet(device):
        pl.semaphore_signal(barrier, inc=1, device_id=device, device_id_type=MESH)

    loop(1, cols, lambda i: greet((row, lax.rem(col + i, cols))))
    greet((other_row, col))

    def greet_if(condition, device):
        @pl.when(condition)
        def _():
            greet(device)

        return condition.astype(jnp.int32)

    greeted = (
        cols
        + greet_if(jnp.logical_not(is_last), (row + 2, col))
        + greet_if(high > 0, (row - 2, col))
        + greet_if(pos + 2 < total, at(pos + 2))
        + greet_if(pos >= 2, at(pos - 2))
    )

    def head_lanes(h, base=0):
        return pl.ds(pl.multiple_of(base + h * DH, DH), DH)

    def remote(src, dst, send, recv, device):
        return pltpu.make_async_remote_copy(
            src_ref=src, dst_ref=dst, send_sem=send, recv_sem=recv,
            device_id=device, device_id_type=MESH,
        )

    def same(ref, send, recv, device):
        return remote(ref, ref, send, recv, device)

    def far_block(r, p):
        return far_buf.at[2 * r + side, pl.ds(pl.multiple_of(p * fars, fars), fars), :]

    def swap(p_to, p_from):
        return same(far_block(row, p_from), swap_send.at[p_to], swap_recv.at[p_from], (row, 2 * p_to + side))

    def side_swap(r, p):
        return same(far_block(r, p), side_send.at[p], side_recv.at[p], beside)

    def up(p):
        return same(far_block(other_row, pair), pass_send.at[p], side_recv.at[pair], (row, 2 * p + side))

    def down(r):
        return same(far_buf.at[2 * r + side], down_send.at[r], down_recv.at[r], (row + 2, col))

    def cross(r):
        return same(far_buf.at[2 * r + side], cross_send.at[lax.rem(r, 2)], down_recv.at[r], beside)

    def lift(r):
        return same(far_buf.at[2 * r + side], lift_send.at[r], down_recv.at[r], (row, col + 2))

    def twin(r, s):
        return same(far_buf.at[2 * r + s], twin_send.at[r], twin_recv.at[r], partner)

    def mid_span(c):
        return mid_buf.at[pl.ds(pl.multiple_of(c * mids, mids), mids), :]

    def mid_copy(p_to, p_from):
        return same(mid_span(2 * p_from + side), mid_sem.at[p_to], mid_sem.at[p_from], (row, 2 * p_to + side))

    def mid_pass(p, s):
        return same(mid_span(2 * p + s), pass_send.at[p], pass_recv.at[p], partner)

    def near_copy(half):
        lanes = pl.ds(pl.multiple_of(half * (KV // 2), KV // 2), KV // 2)
        return remote(
            kv_ref.at[:, :, lanes], near.at[FROM_PARTNER, :, :, lanes],
            own_sem.at[half], own_sem.at[half], partner,
        )

    def behind_copy(h):
        lanes = head_lanes(h)
        return remote(
            kv_ref.at[:, :, lanes], near.at[FROM_BEHIND, :, :, lanes],
            near_send.at[FROM_BEHIND, h], near_recv.at[FROM_BEHIND, h], ahead,
        )

    def relay_copy(h):
        lanes = head_lanes(h)
        return remote(
            near.at[FROM_BEHIND, :, :, lanes], near.at[RELAYED, :, :, lanes],
            near_send.at[RELAYED, h], near_recv.at[RELAYED, h], partner,
        )

    def behind_start(h):
        behind_copy(h).start()

    mid_rows = pl.ds(pl.multiple_of(col * mids, mids), mids)
    far_rows = pl.ds(pl.multiple_of(pair * fars, fars), fars)

    def spread_out(s):
        for h in range(HK):
            wide[s * HK + h] = kv_ref[s, :, h * DH:(h + 1) * DH].astype(jnp.float32)

    def summarise(s, squeeze, weight):
        count = tok // squeeze
        grouped = jnp.concatenate(
            [
                jnp.concatenate(
                    [wide[s * HK + h, pl.ds(i, count, stride=squeeze), :] for h in range(HK)],
                    axis=0,
                ).astype(jnp.bfloat16)
                for i in range(squeeze)
            ],
            axis=1,
        )
        merged = jnp.dot(grouped, weight[...], preferred_element_type=jnp.float32)
        merged = merged.astype(jnp.bfloat16)
        for h in range(HK):
            lanes = slice(s * KV + h * DH, s * KV + (h + 1) * DH)
            piece = merged[h * count:(h + 1) * count]
            if squeeze == FAR:
                far_buf[2 * row + side, far_rows, lanes] = piece
            else:
                mid_buf[mid_rows, lanes] = piece

    def others(f):
        def one(p):
            @pl.when(p != pair)
            def _():
                f(p)

        loop(0, pairs, one)

    def when(condition, f):
        @pl.when(condition)
        def _():
            f()

    for copy in fetches[:2]:
        copy.wait()
    spread_out(0)
    spread_out(1)
    for copy in fetches[2:4]:
        copy.wait()
    summarise(0, FAR, wfk_ref)
    summarise(1, FAR, wfv_ref)
    pl.semaphore_wait(barrier, greeted)
    others(lambda p: swap(p, pair).start())
    side_swap(row, pair).start()
    when(side == 0, lambda: loop(0, 2, lambda half: near_copy(half).start()))
    for copy in fetches[4:6]:
        copy.wait()
    summarise(0, MID, wmk_ref)
    summarise(1, MID, wmv_ref)
    loop(pair + 1, pairs, lambda p: mid_copy(p, pair).start())
    when(side == 0, lambda: mid_pass(pair, 0).start())

    sends = pos + 2 < total
    starts = feeds_beside & (side == 0)
    n_first = jnp.where(is_hub, N_FIRST, HK)

    fetches[6].wait()

    def iota(shape, axis):
        return lax.broadcasted_iota(jnp.int32, shape, axis)

    def query(h, g):
        return q_ref[:, pl.ds(pl.multiple_of((h * GROUP + g) * DH, DH), DH)]

    def near_first(with_partner):
        def two(i):
            seen = iota((tok, tok), 0) <= iota((tok, tok), 1)
            work = []
            if with_partner:
                near_copy(i).wait_recv()
            for h in (2 * i, 2 * i + 1):
                keys = [kv_ref[0, :, head_lanes(h)]]
                flats = [flat(kv_ref[1, :, head_lanes(h)])]
                if with_partner:
                    keys.append(near[FROM_PARTNER, 0, :, head_lanes(h)])
                    flats.append(flat(near[FROM_PARTNER, 1, :, head_lanes(h)]))
                for g in range(GROUP):
                    work.append((h * GROUP + g, [score(k, query(h, g)) for k in keys], flats))
            for n, parts, flats in work:
                parts = [jnp.where(seen, parts[0], NEG_FILL)] + parts[1:]
                top = top_of(parts)
                top_ref[n] = top
                den_ref[n], acc_ref[n] = weigh(parts, top, flats)

        return two

    def spread():
        others(lambda p: side_swap(other_row, p).wait_recv())
        when(jnp.logical_not(is_last), lambda: down(other_row).start())
        when(sends, lambda: loop(n_first, HK, behind_start))
        when(low == 1, lambda: twin(row - 1, side).start())

    def near_more():
        when(sends & starts, lambda: loop(0, HK, behind_start))
        side_swap(other_row, pair).wait_recv()
        loop(pair + 1, pairs, lambda p: up(p).start())

        def over(p):
            swap(p, p).wait_recv()
            side_swap(row, p).start()

        loop(pair + 1, pairs, over)
        loop(0, pair, lambda p: swap(p, p).wait_recv())
        when(sends & jnp.logical_not(starts), lambda: loop(0, n_first, behind_start))
        when(jnp.logical_not(is_last), lambda: down(row).start())

    def near_own(with_partner):
        two = near_first(with_partner)

        def step(i):
            if with_partner:
                when(i == 0, near_more)
            two(i)
            if with_partner:
                when(i == 0, spread)
            else:
                when(i == 0, near_more)
                when(i == 1, spread)

        loop(0, HK // 2, step)

    @pl.when(side == 0)
    def _():
        near_own(False)

    @pl.when(side == 1)
    def _():
        near_own(True)

    def mid_arrive(p):
        mid_copy(p, p).wait_recv()
        mid_pass(p, side).start()

    loop(0, pair, mid_arrive)
    loop(0, pair, lambda p: mid_pass(p, 1 - side).wait_recv())

    @pl.when(side == 1)
    def _():
        mid_pass(pair, 0).wait_recv()

    n_mid = mid_buf.shape[0]

    def mid_all():
        seen = (iota((n_mid, tok), 0) * MID + MID - 1) <= (iota((n_mid, tok), 1) + col * tok)
        work = []
        for h in range(HK):
            keys = mid_buf[:, head_lanes(h)]
            values = flat(mid_buf[:, head_lanes(h, KV)])
            for g in range(GROUP):
                work.append((h * GROUP + g, score(keys, query(h, g)), values))
        for n, s, values in work:
            s = jnp.where(seen, s, NEG_FILL)
            den, acc = weigh([s], jnp.maximum(top_of([s]), TOP_FLOOR), [values])
            rest_ref[n] = acc * inverse(den)

    mid_all()

    def hand_on(k):
        def one(i):
            r = 2 * (high - 1 - k) + lax.rem(low + i, 2)

            @pl.when(is_hub)
            def _():
                when(k == 0, lambda: down(r).wait_recv())
                when(k == 1, lambda: cross(r).wait_recv())
                when(k > 1, lambda: lift(r).wait_recv())

            @pl.when(jnp.logical_not(is_hub))
            def _():
                down(r).wait_recv()
                when(jnp.logical_not(is_last), lambda: down(r).start())
                when(feeds_beside & (k == 1), lambda: cross(r).start())
                when(feeds_next & (k > 1), lambda: lift(r).start())

            twin(r, side).start()

        loop(0, 2, one)

    def arrive(h):
        behind_copy(h).wait_recv()
        relay_copy(h).start()

    def near_last(h, last=False):
        relay_copy(h).wait_recv()
        slots = (FROM_BEHIND, RELAYED)
        keys = [near[slot, 0, :, head_lanes(h)] for slot in slots]
        flats = [flat(near[slot, 1, :, head_lanes(h)]) for slot in slots]
        work = [[score(k, query(h, g)) for k in keys] for g in range(GROUP)]
        for g, parts in enumerate(work):
            n = h * GROUP + g
            before = top_ref[n]
            top = jnp.maximum(before, top_of(parts))
            den, acc = weigh(parts, top, flats)
            fade = powers(before, top)
            den, acc = den_ref[n] * fade + den, acc_ref[n] * fade + acc
            if last:
                put(n, acc * inverse(den) + rest_ref[n] + far_acc[n] * inverse(far_den[n]))
            else:
                den_ref[n], acc_ref[n] = den, acc

    line = far_buf.shape[1]
    def put(n, whole):
        lanes = pl.ds(pl.multiple_of(n * DH, DH), DH)
        out_ref[:, lanes] = whole.astype(out_ref.dtype).T

    def far_chunk(j, last=False):
        def part(h, base):
            block = far_buf[pl.ds(j * SLABS, SLABS), :, head_lanes(h, base)]
            return block.reshape(SLABS * line, DH)

        seen = iota((SLABS * line, 1), 0) + j * (SLABS * line) < 2 * row * line
        work = []
        for h in range(HK):
            keys, flats = part(h, 0), flat(part(h, KV))
            work += [(h * GROUP + g, score(keys, query(h, g)), flats) for g in range(GROUP)]
        for n, s, flats in work:
            s = jnp.where(seen, s, NEG_FILL)
            before = far_top[n]
            top = jnp.maximum(before, top_of([s]))
            fade = powers(before, top)
            den, acc = weigh([s], top, [flats])
            den, acc = far_den[n] * fade + den, far_acc[n] * fade + acc
            if last:
                put(n, acc_ref[n] * inverse(den_ref[n]) + rest_ref[n] + acc * inverse(den))
            else:
                far_top[n], far_den[n], far_acc[n] = top, den, acc

    def far_rows(j, last=False):
        loop(2 * j, jnp.minimum(2 * j + 2, row), lambda r: twin(r, 1 - side).wait_recv())
        far_chunk(j, last)

    def far_back(k_low, k_high):
        loop(k_low, k_high, lambda k: far_rows(high - 1 - k))

    def finish(with_far, h):
        for g in range(GROUP):
            n = h * GROUP + g
            whole = acc_ref[n] * inverse(den_ref[n]) + rest_ref[n]
            if with_far:
                whole = whole + far_acc[n] * inverse(far_den[n])
            put(n, whole)

    def sent_early():
        others(lambda p: swap(p, pair).wait_send())
        loop(pair + 1, pairs, lambda p: mid_copy(p, pair).wait_send())
        loop(pair, pairs, lambda p: side_swap(row, p).wait_send())
        loop(pair + 1, pairs, lambda p: up(p).wait_send())
        loop(0, pair, lambda p: mid_pass(p, side).wait_send())

        @pl.when(side == 0)
        def _():
            loop(0, 2, lambda half: near_copy(half).wait_send())
            mid_pass(pair, 0).wait_send()

    def feeds_next_done():
        @pl.when(jnp.logical_not(is_last))
        def _():
            loop(jnp.where(is_hub, 2 * high, 0), 2 * high + 2, lambda r: down(r).wait_send())

        @pl.when(feeds_beside & (high > 1))
        def _():
            loop(2 * high - 4, 2 * high - 2, lambda r: cross(r).wait_send())

        @pl.when(feeds_next)
        def _():
            loop(0, 2 * high - 4, lambda r: lift(r).wait_send())

    def near_in(h):
        when(pos >= 2, lambda: arrive(h))

    def near_end(h):
        @pl.when(pos >= 2)
        def _():
            near_last(h)

    plain = jnp.logical_not(is_hub)
    near_late = (low == 0) & (pair == 0) & (side == 0) & (high > 1)
    far_late = (low == 0) & (pair == 0) & (high > 1) & jnp.logical_not(is_last)

    ends_near = plain & (row > 0)

    def step(s):
        when((s == 0) & (high > 0) & plain, lambda: hand_on(0))
        when((s < HK) & (s != 2), lambda: near_in(s))
        when(s == 0, lambda: far_back(jnp.where(low == 1, -1, 0), jnp.where(plain & jnp.logical_not(far_late), jnp.minimum(high, 1), 0)))
        when((s == 1) & (high > 1) & plain, lambda: hand_on(1))
        when((s > 0) & jnp.logical_not(ends_near & (s == HK)), lambda: near_end(s - 1))

        @pl.when(s == 2)
        def _():
            loop(jnp.where(is_hub, 0, 2), jnp.where(is_hub, jnp.minimum(high, 1), high), hand_on)
            first = jnp.where(plain & jnp.logical_not(far_late), 1, 0)
            split = jnp.where(near_late, first + 1, first)
            far_back(first, split)
            near_in(2)
            far_back(split, jnp.where(plain, high, jnp.minimum(high, 1)))
            when((row > 0) & plain, lambda: loop(0, 2, functools.partial(finish, True)))

        @pl.when(s == HK - 1)
        def _():
            sent_early()
            when(is_hub & (high > 1), lambda: hand_on(1))
            when(plain & (row > 0), lambda: loop(2, HK - 1, functools.partial(finish, True)))

    loop(0, HK + 1, step)
    when(ends_near, lambda: near_last(HK - 1, True))

    @pl.when(row > 0)
    def _():
        ends_far = is_hub & (high > 1)

        @pl.when(ends_far)
        def _():
            loop(2, high, hand_on)
            far_back(1, high - 1)
            far_rows(0, True)

        @pl.when(is_hub & jnp.logical_not(ends_far))
        def _():
            loop(0, HK, functools.partial(finish, True))

    @pl.when(row == 0)
    def _():
        loop(0, HK, functools.partial(finish, False))

    loop(0, row, lambda r: twin(r, side).wait_send())
    feeds_next_done()

    @pl.when(pos + 2 < total)
    def _():
        loop(0, HK, lambda h: behind_copy(h).wait_send())

    @pl.when(pos >= 2)
    def _():
        loop(0, HK, lambda h: relay_copy(h).wait_send())


def body(rows, cols, queries, keys, values, *weights):
    tok = queries.shape[0]
    assert BLOCK == 2 * tok and cols % 2 == 0 and rows % 2 == 0
    dma = pltpu.SemaphoreType.DMA
    bf16, f32 = jnp.bfloat16, jnp.float32
    vmem = pl.BlockSpec(memory_space=pltpu.VMEM)
    pairs = cols // 2
    return pl.pallas_call(
        functools.partial(kernel, rows, cols),
        out_shape=pltpu.VMEM(queries.shape, bf16),
        in_specs=[pl.BlockSpec(memory_space=pltpu.HBM)] * 7,
        out_specs=vmem,
        scratch_shapes=[
            pltpu.VMEM(queries.shape, bf16),
            pltpu.VMEM((2, *keys.shape), bf16),
            *[pltpu.VMEM(a.shape, a.dtype) for a in weights],
            dma((7,)),
            pltpu.VMEM((2 * HK, tok, DH), f32),
            pltpu.VMEM((cols * (tok // MID), 2 * KV), bf16),
            pltpu.VMEM((2 * rows, pairs * (tok // FAR), 2 * KV), bf16),
            pltpu.VMEM((3, 2, tok, KV), bf16),
            pltpu.VMEM((HQ, 1, tok), f32),
            pltpu.VMEM((HQ, 1, tok), f32),
            pltpu.VMEM((HQ, DH, tok), f32),
            pltpu.VMEM((HQ, DH, tok), f32),
            pltpu.VMEM((HQ, 1, tok), f32),
            pltpu.VMEM((HQ, 1, tok), f32),
            pltpu.VMEM((HQ, DH, tok), f32),
            dma((2, HK)),
            dma((2, HK)),
            dma((2,)),
            *[dma((pairs,))] * 7,
            *[dma((rows,))] * 2,
            dma((2,)),
            dma((max(rows - 6, 1),)),
            *[dma((rows,))] * 2,
        ],
        compiler_params=pltpu.CompilerParams(
            collective_id=0, has_side_effects=True, vmem_limit_bytes=VMEM_LIMIT
        ),
    )(queries, keys, values, *weights)


def solution(mesh):
    spec = P(("row", "col"), None)
    return jax.shard_map(
        functools.partial(body, mesh.shape["row"], mesh.shape["col"]),
        mesh=mesh,
        in_specs=(spec, spec, spec, P(), P(), P(), P()),
        out_specs=spec,
        check_vma=False,
    )
```
